256 devices in a mesh: lat: 16 (over z, core), lon: 8 (over x, y_hi), ens: 2 (over y_lo).
Axes of the slice: x: 4, y: 4 (y_hi: 2, y_lo: 2; y = y_hi * 2 + y_lo), z: 8, core: 2. Of those that a mesh axis runs over, the one named last changes fastest.
Arguments:
- state: bfloat16 [4, 96, 192, 768], P('ens', 'lat', 'lon'), parts along dimension 0, may hold values from -6 to 6
- spec_weight1: float32 [2, 8, 96, 96], P(None, 'lon'), may hold values from -0.4375 to 0.4375
- spec_bias1: float32 [2, 8, 96], P(None, 'lon'), may hold values from -0.6 to 0.6
- spec_weight2: float32 [2, 8, 96, 96], P(None, 'lon'), may hold values from -0.4375 to 0.4375
- spec_bias2: float32 [2, 8, 96], P(None, 'lon'), may hold values from -0.12 to 0.12
- norm1_gain: float32 [768], replicated, may hold values from 0.5 to 1.5
- norm1_bias: float32 [768], replicated, may hold values from -0.6 to 0.6
- norm2_gain: float32 [768], replicated, may hold values from 0.5 to 1.5
- norm2_bias: float32 [768], replicated, may hold values from -0.6 to 0.6
- fc1_weight: bfloat16 [768, 3072], replicated, may hold values from -0.21875 to 0.21875
- fc1_bias: float32 [3072], replicated, may hold values from -0.6 to 0.6
- fc2_weight: bfloat16 [3072, 768], replicated, may hold values from -0.109375 to 0.109375
- fc2_bias: float32 [768], replicated, may hold values from -0.6 to 0.6
- cotangent: bfloat16 [4, 96, 192, 768], P('ens', 'lat', 'lon'), parts along dimension 0, may hold values from -6 to 6
Outputs:
- advanced: bfloat16 [4, 96, 192, 768], P('ens', 'lat', 'lon'), parts along dimension 0
- sensitivity: bfloat16 [4, 96, 192, 768], P('ens', 'lat', 'lon'), parts along dimension 0
The draws below stay inside these ranges and needn't reach their ends.
There are 2 independent parts, one for each index of `ens`. The reference program is written for one: setup_inputs(seed, part) draws one part's arguments, and reference() takes and returns one part's arrays. A program takes and returns all parts, laid end to end along the dimension named above; an argument that names none is the same for every part. Nothing has to cross between parts.
All inputs are finite; a program needn't handle non-finite values.
Results may differ from the reference program's by a relative error of at most 0.0085.
Values may be sent and summed in bfloat16 or wider, within the bound.
No kernel may reach another device: no remote copies, remote signals or barrier semaphores. Data moves between devices by JAX's collectives and lax.ppermute only.
A program may use at most 128 MiB of HBM per device.

```python
import jax
import jax.numpy as jnp
from jax import lax

D = 768
FF = 3072
NB = 8
BS = 96
B = 2
H = 96
W = 192


def steps_of(stream_key, extent, cuts, least, largest):
    loudness, own = 1.0, jax.random.fold_in(stream_key, 6)
    for position, shards_of in cuts:
        steps = jnp.exp(jax.random.uniform(jax.random.fold_in(own, position), (shards_of,), jnp.float32, least / len(cuts), largest / len(cuts)))
        loudness = loudness * jnp.repeat(steps, extent[position] // shards_of).reshape([-1 if axis == position else 1 for axis in range(len(extent))])
    return loudness


def scatter_about(own_key, extent, spread, limit, shards=(), kind=jnp.bfloat16):
    drawn = jax.random.normal(own_key, extent, jnp.float32) * spread
    if len(shards) > 0:
        drawn = steps_of(own_key, extent, shards, -0.22, 0.18) * drawn
    return jnp.clip(drawn, min=-limit, max=limit).astype(kind)


def setup_inputs(seed: int = 0, part: int = 0) -> dict:
    streams_of = jax.random.split(jax.random.key(seed), 15)
    part_splits = jax.random.split(jax.random.fold_in(streams_of[14], part), 15)
    return {
        "state": scatter_about(part_splits[0], (B, H, W, D), 1.0, 6.0, ((1, 16), (2, 8))),
        "spec_weight1": scatter_about(streams_of[1], (2, NB, BS, BS), (2 * BS) ** -0.5, 0.4375, ((1, 8),), jnp.float32),
        "spec_bias1": scatter_about(streams_of[2], (2, NB, BS), 0.1, 0.6, ((1, 8),), jnp.float32),
        "spec_weight2": scatter_about(streams_of[3], (2, NB, BS, BS), (2 * BS) ** -0.5, 0.4375, ((1, 8),), jnp.float32),
        "spec_bias2": scatter_about(streams_of[4], (2, NB, BS), 0.02, 0.12, ((1, 8),), jnp.float32),
        "norm1_gain": jnp.clip(1.0 + 0.1 * jax.random.normal(streams_of[5], (D,), jnp.float32), 0.5, 1.5),
        "norm1_bias": scatter_about(streams_of[6], (D,), 0.1, 0.6, (), jnp.float32),
        "norm2_gain": jnp.clip(1.0 + 0.1 * jax.random.normal(streams_of[7], (D,), jnp.float32), 0.5, 1.5),
        "norm2_bias": scatter_about(streams_of[8], (D,), 0.1, 0.6, (), jnp.float32),
        "fc1_weight": scatter_about(streams_of[9], (D, FF), D ** -0.5, 0.21875),
        "fc1_bias": scatter_about(streams_of[10], (FF,), 0.1, 0.6, (), jnp.float32),
        "fc2_weight": scatter_about(streams_of[11], (FF, D), FF ** -0.5, 0.109375),
        "fc2_bias": scatter_about(streams_of[12], (D,), 0.1, 0.6, (), jnp.float32),
        "cotangent": scatter_about(part_splits[13], (B, H, W, D), 1.0, 6.0, ((1, 16), (2, 8))),
    }


HIGH = lax.Precision.HIGHEST
EPSILON = 1e-06
THRESHOLD = 0.01

def layer_norm(values, gain, shift):
    average = lax.optimization_barrier(jnp.mean(values, axis=-1, keepdims=True))
    centred = values - average
    inverse = lax.rsqrt(lax.optimization_barrier(jnp.mean(centred * centred, axis=-1, keepdims=True)) + EPSILON)
    normed = centred * inverse
    return (normed * gain + shift, normed, inverse)

def norm_backward(gradient, gain, normed, inverse):
    scaled = gradient * gain
    return inverse * (scaled - lax.optimization_barrier(jnp.mean(scaled, axis=-1, keepdims=True)) - normed * lax.optimization_barrier(jnp.mean(scaled * normed, axis=-1, keepdims=True)))

def gelu_exact(values):
    return jax.nn.gelu(values, approximate=False)

def gelu_slope(values):
    cumulative = 0.5 * (1.0 + lax.erf(values * 0.7071067811865476))
    density = jnp.exp(-0.5 * values * values) * 0.3989422804014327
    return cumulative + values * density

def block_product(real_part, imag_part, weight):
    blocks, width = (weight.shape[1], weight.shape[2])
    shape = real_part.shape
    real_split = real_part.reshape(shape[:-1] + (blocks, width))
    imag_split = imag_part.reshape(shape[:-1] + (blocks, width))

    def multiply(values, matrix):
        return jnp.einsum('...nb,nbo->...no', values, matrix, precision=HIGH).reshape(shape)
    return (multiply(real_split, weight[0]) - multiply(imag_split, weight[1]), multiply(real_split, weight[1]) + multiply(imag_split, weight[0]))

def block_adjoint(real_part, imag_part, weight):
    blocks, width = (weight.shape[1], weight.shape[2])
    shape = real_part.shape
    real_split = real_part.reshape(shape[:-1] + (blocks, width))
    imag_split = imag_part.reshape(shape[:-1] + (blocks, width))

    def multiply(values, matrix):
        return jnp.einsum('...no,nbo->...nb', values, matrix, precision=HIGH).reshape(shape)
    return (multiply(real_split, weight[0]) + multiply(imag_split, weight[1]), multiply(imag_split, weight[0]) - multiply(real_split, weight[1]))

def forward_transform(field):
    spectrum = jnp.fft.fft2(field, axes=(1, 2), norm='ortho')
    return (jnp.real(spectrum), jnp.imag(spectrum))

def inverse_real(real_part, imag_part):
    return jnp.real(jnp.fft.ifft2(lax.complex(real_part, imag_part), axes=(1, 2), norm='ortho'))

def reference(state, spec_weight1, spec_bias1, spec_weight2, spec_bias2, norm1_gain, norm1_bias, norm2_gain, norm2_bias, fc1_weight, fc1_bias, fc2_weight, fc2_bias, cotangent):
    source = state.astype(jnp.float32)
    normed_one, hat_one, inverse_one = layer_norm(source, norm1_gain, norm1_bias)
    lowered = normed_one.astype(jnp.bfloat16)
    spec_real, spec_imag = forward_transform(lowered.astype(jnp.float32))
    first_real, first_imag = block_product(spec_real, spec_imag, spec_weight1)
    first_real = first_real + spec_bias1[0].reshape(-1)
    first_imag = first_imag + spec_bias1[1].reshape(-1)
    second_real, second_imag = block_product(gelu_exact(first_real), gelu_exact(first_imag), spec_weight2)
    second_real = second_real + spec_bias2[0].reshape(-1)
    second_imag = second_imag + spec_bias2[1].reshape(-1)
    shrunk_real = second_real - THRESHOLD * jnp.tanh(second_real / THRESHOLD)
    shrunk_imag = second_imag - THRESHOLD * jnp.tanh(second_imag / THRESHOLD)
    filtered = inverse_real(shrunk_real, shrunk_imag)
    mixed = (filtered + lowered.astype(jnp.float32) + source).astype(jnp.bfloat16)

    def token_rows(row_pair):
        mixed_rows, cot_rows = row_pair
        mixed_float = mixed_rows.astype(jnp.float32)
        normed_two, hat_two, inverse_two = layer_norm(mixed_float, norm2_gain, norm2_bias)
        hidden_pre = jnp.dot(normed_two.astype(jnp.bfloat16), fc1_weight, preferred_element_type=jnp.float32) + fc1_bias
        hidden = gelu_exact(hidden_pre).astype(jnp.bfloat16)
        advanced_rows = (jnp.dot(hidden, fc2_weight, preferred_element_type=jnp.float32) + fc2_bias + mixed_float).astype(jnp.bfloat16)
        grad_hidden = jnp.dot(cot_rows, fc2_weight.T, preferred_element_type=jnp.float32)
        grad_pre = (grad_hidden * gelu_slope(hidden_pre)).astype(jnp.bfloat16)
        grad_normed = jnp.dot(grad_pre, fc1_weight.T, preferred_element_type=jnp.float32)
        grad_rows = (cot_rows.astype(jnp.float32) + norm_backward(grad_normed, norm2_gain, hat_two, inverse_two)).astype(jnp.bfloat16)
        return (advanced_rows, grad_rows)
    row_shape = (-1,) + mixed.shape[2:]
    advanced, grad_mixed = lax.map(token_rows, (mixed.reshape(row_shape), cotangent.reshape(row_shape)))
    advanced = advanced.reshape(state.shape)
    grad_mixed = grad_mixed.reshape(state.shape)
    grad_float = grad_mixed.astype(jnp.float32)
    gs_real, gs_imag = forward_transform(grad_float)
    slope_real = jnp.tanh(second_real / THRESHOLD)
    slope_imag = jnp.tanh(second_imag / THRESHOLD)
    gq_real = gs_real * slope_real * slope_real
    gq_imag = gs_imag * slope_imag * slope_imag
    ga_real, ga_imag = block_adjoint(gq_real, gq_imag, spec_weight2)
    gp_real = ga_real * gelu_slope(first_real)
    gp_imag = ga_imag * gelu_slope(first_imag)
    gz_real, gz_imag = block_adjoint(gp_real, gp_imag, spec_weight1)
    grad_lowered = inverse_real(gz_real, gz_imag) + grad_float
    sensitivity = (grad_float + norm_backward(grad_lowered, norm1_gain, hat_one, inverse_one)).astype(jnp.bfloat16)
    return (advanced, sensitivity)
```

```python
import functools
import math

import jax
import jax.numpy as jnp
import numpy as np
from jax import lax
from jax.experimental import pallas as pl
from jax.experimental.pallas import tpu as pltpu
from jax.sharding import PartitionSpec as P

EPSILON = 1e-06
THRESHOLD = 0.01
LATS, LONS = 16, 8
HEIGHT, WIDTH, FEATURES, HIDDEN = 96, 192, 768, 3072
ROWS, COLS = HEIGHT // LATS, WIDTH // LONS
BLOCK = FEATURES // LONS
STATES = 2
GROUPS = STATES * ROWS
TOKENS = GROUPS * COLS
LANES = GROUPS * BLOCK
TILES = LANES // 128
WIRE = TILES * GROUPS
STRIDE = 109
CHUNK = 512
F32, BF16 = jnp.float32, jnp.bfloat16


def split_table(table):
    high = table.astype(BF16)
    return np.stack([high, (table - high.astype(np.float64)).astype(BF16)])


def width_tables():
    part, q, d = np.meshgrid(np.arange(2), np.arange(ROWS), np.arange(LATS), indexing="ij")
    part, freq = part.reshape(-1, 1), (q + ROWS * d).reshape(-1, 1)
    w = np.arange(WIDTH).reshape(1, -1)
    angle = 2.0 * math.pi * (freq * w % WIDTH) / WIDTH
    parity = np.where(w % 2 == 0, 1.0, -1.0)
    scale = 1.0 / math.sqrt(WIDTH)
    forward = np.where(part == 0, np.cos(angle), np.where(freq == 0, parity, -np.sin(angle)))
    twice = np.where(freq == 0, 1.0, 2.0)
    return forward * scale, (forward * twice * scale).T


def height_tables():
    p = np.arange(HEIGHT).reshape(-1, 1, 1)
    r = np.arange(ROWS).reshape(1, -1, 1)
    s = np.arange(LATS).reshape(1, 1, -1)
    angle = 2.0 * math.pi * (p * (ROWS * s + r) % HEIGHT) / HEIGHT
    c, n = np.cos(angle) / math.sqrt(HEIGHT), np.sin(angle) / math.sqrt(HEIGHT)
    zero = np.zeros_like(c)

    def join(rows):
        return np.concatenate([np.stack(row, axis=2).reshape(HEIGHT, -1) for row in rows], axis=0)

    plain = join([[c, n], [c, n], [-n, c], [n, -c]])
    packed = join([[c, zero], [zero, c], [-n, zero], [zero, -n]])

    def join_back(rows):
        return np.concatenate(
            [np.concatenate([v.reshape(HEIGHT, -1).T for v in row], axis=1) for row in rows], axis=0
        )

    h = 0.5
    plain_back = join_back([[h * c, h * c, -h * n, h * n], [h * n, h * n, h * c, -h * c]])
    packed_back = join_back([[c, zero, -n, zero], [zero, c, zero, -n]])
    return np.stack([plain, packed]), np.stack([plain_back, packed_back])


def dot(a, b):
    return lax.dot_general(a, b, (((1,), (0,)), ((), ())), preferred_element_type=F32)


def dot_t(a, b):
    return lax.dot_general(a, b, (((1,), (1,)), ((), ())), preferred_element_type=F32)


def lane_index(rows):
    return lax.broadcasted_iota(jnp.int32, (rows, 128), 1)


def unpack4(t0, t1, t2):
    lane = lane_index(t0.shape[0])
    b1 = jnp.where(lane < 32, pltpu.roll(t0, 32, 1), pltpu.roll(t1, 32, 1))
    b2 = jnp.where(lane < 64, pltpu.roll(t1, 64, 1), pltpu.roll(t2, 64, 1))
    return t0, b1, b2, pltpu.roll(t2, 96, 1)


def pack4(b0, b1, b2, b3):
    lane = lane_index(b0.shape[0])
    r1, r2, r3 = pltpu.roll(b1, 96, 1), pltpu.roll(b2, 64, 1), pltpu.roll(b3, 32, 1)
    return (
        jnp.where(lane < 96, b0, r1),
        jnp.where(lane < 64, r1, r2),
        jnp.where(lane < 32, r2, r3),
    )


def norm(values):
    average = jnp.mean(values, axis=-1, keepdims=True)
    centred = values - average
    inverse = lax.rsqrt(jnp.mean(centred * centred, axis=-1, keepdims=True) + EPSILON)
    return centred * inverse, inverse


def norm_backward(gradient, gain, normed, inverse):
    scaled = gradient * gain
    return inverse * (
        scaled
        - jnp.mean(scaled, axis=-1, keepdims=True)
        - normed * jnp.mean(scaled * normed, axis=-1, keepdims=True)
    )


def gelu_pair(values):
    cumulative = 0.5 * (1.0 + lax.erf(values * 0.7071067811865476))
    density = jnp.exp(-0.5 * values * values) * 0.3989422804014327
    return values * cumulative, cumulative + values * density


def scatter_blocks(blocks, pair, values):
    tiles = [values[:, 128 * i : 128 * i + 128] for i in range(6)]
    for j, b in enumerate((*unpack4(*tiles[:3]), *unpack4(*tiles[3:]))):
        blocks[j, 2 * pair] = b[:COLS]
        blocks[j, 2 * pair + 1] = b[COLS:]


def send_blocks(blocks, wire):
    for j in range(LONS):
        for g in range(GROUPS // 4):
            tiles = pack4(*(blocks[j, 4 * g + n] for n in range(4)))
            for i, t in enumerate(tiles):
                at = 384 * g + 128 * i
                wire[j, :, at : at + 128] = t.astype(BF16)


def receive_blocks(wire, blocks):
    for j in range(LONS):
        for g in range(GROUPS // 4):
            at = 384 * g
            tiles = [wire[j, :, at + 128 * i : at + 128 * i + 128].astype(F32) for i in range(3)]
            for n, b in enumerate(unpack4(*tiles)):
                blocks[j, 4 * g + n] = b


def gather_blocks(blocks, pair):
    parts = [jnp.concatenate([blocks[j, 2 * pair], blocks[j, 2 * pair + 1]], axis=0) for j in range(LONS)]
    return jnp.concatenate([*pack4(*parts[:4]), *pack4(*parts[4:])], axis=1)


def begin_kernel(state, gain, shift, lowered, wire, blocks):
    for pair in range(GROUPS // 2):
        rows = slice(48 * pair, 48 * pair + 48)
        normed, _ = norm(state[rows, :].astype(F32))
        value = (normed * gain[...] + shift[...]).astype(BF16)
        lowered[rows, :] = value
        scatter_blocks(blocks, pair, value.astype(F32))
    send_blocks(blocks, wire)


def wire_out(scratch, wire):
    for d in range(LATS):
        wire[d] = scratch[STRIDE * d : STRIDE * d + WIRE, :].astype(BF16)


def wire_in(wire, scratch):
    for d in range(LATS):
        scratch[STRIDE * d : STRIDE * d + WIRE, :] = wire[d].astype(F32)


def peers(row):
    return pl.ds(row, LATS, stride=STRIDE)


def width_kernel(field, table, wire, scratch):
    product = dot(table[0], field[...]) + dot(table[1], field[...])
    for e in range(GROUPS):
        for i in range(TILES):
            scratch[peers(GROUPS * i + e), :] = product[16 * e : 16 * e + 16, 128 * i : 128 * i + 128]
    wire_out(scratch, wire)


def width_back_kernel(wire, table, field, scratch, gathered):
    wire_in(wire, scratch)
    for e in range(GROUPS):
        for i in range(TILES):
            piece = scratch[peers(GROUPS * i + e), :]
            gathered[16 * e : 16 * e + 16, 128 * i : 128 * i + 128] = piece.astype(BF16)
    field[...] = (dot(table[0], gathered[...]) + dot(table[1], gathered[...])).astype(BF16)


def spectrum_in(wire, scratch, columns):
    wire_in(wire, scratch)
    for part in range(2):
        for q in range(ROWS):
            e = ROWS * part + q
            for g in range(GROUPS // 4):
                tiles = [scratch[peers(GROUPS * (3 * g + i) + e), :] for i in range(3)]
                for n, b in enumerate(unpack4(*tiles)):
                    state, r = divmod(4 * g + n, ROWS)
                    at = 16 * (2 * r + part)
                    columns[q, at : at + 16, 128 * state : 128 * state + 128] = b.astype(BF16)


def spectrum_out(backs, scratch, wire):
    for part in range(2):
        for q in range(ROWS):
            e = ROWS * part + q
            for g in range(GROUPS // 4):
                blocks = []
                for n in range(4):
                    state, r = divmod(4 * g + n, ROWS)
                    at = 16 * (ROWS * part + r)
                    blocks.append(backs[q, at : at + 16, 128 * state : 128 * state + 128])
                for i, t in enumerate(pack4(*blocks)):
                    scratch[peers(GROUPS * (3 * g + i) + e), :] = t
    wire_out(scratch, wire)


def build_weight(weight, square, out):
    square[...] = jnp.zeros_like(square)
    square[0:BLOCK, 0:BLOCK] = weight[0]
    square[0:BLOCK, 128 : 128 + BLOCK] = weight[1]
    square[128 : 128 + BLOCK, 0:BLOCK] = -weight[1]
    square[128 : 128 + BLOCK, 128 : 128 + BLOCK] = weight[0]
    full = square[...]
    high = full.astype(BF16)
    out[0] = high
    out[1] = (full - high.astype(F32)).astype(BF16)


def build_bias(bias, out):
    out[...] = jnp.zeros_like(out)
    out[0:1, 0:BLOCK] = bias[0:1, :]
    out[0:1, 128 : 128 + BLOCK] = bias[1:2, :]


def to_points(spectrum):
    half = 2 * HEIGHT
    return jnp.concatenate(
        [
            jnp.concatenate([spectrum[:half, at : at + 128], spectrum[half:, at : at + 128]], axis=1)
            for at in (0, 128)
        ],
        axis=0,
    )


def from_points(points):
    half = 2 * HEIGHT
    return jnp.concatenate(
        [
            jnp.concatenate([points[at : at + half, :128], points[at : at + half, 128:]], axis=0)
            for at in (0, half)
        ],
        axis=1,
    )


def filter_kernel(
    wire, forward, inverse, weight1, bias1, weight2, bias2,
    wire_back, slopes, squares,
    scratch, columns, backs, square, w1, w2, c1, c2,
):
    build_weight(weight1, square, w1)
    build_weight(weight2, square, w2)
    build_bias(bias1, c1)
    build_bias(bias2, c2)
    spectrum_in(wire, scratch, columns)
    first = jnp.where(lax.axis_index("lat") == 0, 1, 0)

    def column(q, which):
        field = columns[q]
        spectrum = dot(forward[which, 0], field) + dot(forward[which, 1], field)
        points = to_points(spectrum.astype(BF16))
        pre = dot(points, w1[0]) + dot(points, w1[1]) + c1[...]
        active, slope = gelu_pair(pre)
        slopes[q] = slope.astype(BF16)
        active = active.astype(BF16)
        post = dot(active, w2[0]) + dot(active, w2[1]) + c2[...]
        bend = jnp.tanh(post * (1.0 / THRESHOLD))
        squares[q] = (bend * bend).astype(BF16)
        shrunk = from_points((post - THRESHOLD * bend).astype(BF16))
        backs[q] = dot(inverse[which, 0], shrunk) + dot(inverse[which, 1], shrunk)

    column(0, first)

    @pl.loop(1, ROWS)
    def _(q):
        column(q, 0)

    spectrum_out(backs, scratch, wire_back)


def adjoint_kernel(
    wire, forward, inverse, weight1, weight2, slopes, squares,
    wire_back,
    scratch, columns, backs, square, w1, w2,
):
    build_weight(weight1, square, w1)
    build_weight(weight2, square, w2)
    spectrum_in(wire, scratch, columns)
    first = jnp.where(lax.axis_index("lat") == 0, 1, 0)

    def column(q, which):
        field = columns[q]
        spectrum = dot(forward[which, 0], field) + dot(forward[which, 1], field)
        points = (to_points(spectrum) * squares[q].astype(F32)).astype(BF16)
        active = dot_t(points, w2[0]) + dot_t(points, w2[1])
        pre = (active * slopes[q].astype(F32)).astype(BF16)
        result = dot_t(pre, w1[0]) + dot_t(pre, w1[1])
        shrunk = from_points(result.astype(BF16))
        backs[q] = dot(inverse[which, 0], shrunk) + dot(inverse[which, 1], shrunk)

    column(0, first)

    @pl.loop(1, ROWS)
    def _(q):
        column(q, 0)

    spectrum_out(backs, scratch, wire_back)


def token_kernel(
    wire, state, lowered, cotangent, gain, shift, fc1, bias1, fc2, bias2,
    advanced, grad_mixed, wire_next,
    blocks, mixed, rows_in, total, grad_total,
):
    step = pl.program_id(0)

    @pl.when(step == 0)
    def _():
        receive_blocks(wire, blocks)
        for pair in range(GROUPS // 2):
            rows = slice(48 * pair, 48 * pair + 48)
            value = gather_blocks(blocks, pair)
            value = value + lowered[rows, :].astype(F32) + state[rows, :].astype(F32)
            value = value.astype(BF16)
            mixed[rows, :] = value
            normed, _ = norm(value.astype(F32))
            rows_in[rows, :] = (normed * gain[...] + shift[...]).astype(BF16)
        total[...] = jnp.zeros_like(total)
        grad_total[...] = jnp.zeros_like(grad_total)

    hidden_pre = dot(rows_in[...], fc1[...]) + bias1[...]
    hidden, slope = gelu_pair(hidden_pre)
    total[...] += dot(hidden.astype(BF16), fc2[...])
    grad_hidden = dot_t(cotangent[...], fc2[...])
    grad_pre = (grad_hidden * slope).astype(BF16)
    grad_total[...] += dot_t(grad_pre, fc1[...])

    @pl.when(step == pl.num_programs(0) - 1)
    def _():
        for pair in range(GROUPS // 2):
            rows = slice(48 * pair, 48 * pair + 48)
            value = mixed[rows, :].astype(F32)
            normed, scale = norm(value)
            advanced[rows, :] = (total[rows, :] + bias2[...] + value).astype(BF16)
            grad = cotangent[rows, :].astype(F32) + norm_backward(
                grad_total[rows, :], gain[...], normed, scale
            )
            grad = grad.astype(BF16)
            grad_mixed[rows, :] = grad
            scatter_blocks(blocks, pair, grad.astype(F32))
        send_blocks(blocks, wire_next)


def finish_kernel(wire, grad_mixed, state, gain, sensitivity, blocks):
    receive_blocks(wire, blocks)
    for pair in range(GROUPS // 2):
        rows = slice(48 * pair, 48 * pair + 48)
        grad = grad_mixed[rows, :].astype(F32)
        normed, scale = norm(state[rows, :].astype(F32))
        grad_lowered = gather_blocks(blocks, pair) + grad
        sensitivity[rows, :] = (grad + norm_backward(grad_lowered, gain[...], normed, scale)).astype(BF16)


def array(shape, dtype=BF16):
    return jax.ShapeDtypeStruct(shape, dtype)


LON_WIRE = array((LONS, COLS, LANES))
LAT_WIRE = array((LATS, WIRE, 128))
BLOCKS = pltpu.VMEM((LONS, GROUPS, COLS, 128), F32)
PEERS = pltpu.VMEM((LATS * STRIDE + 7, 128), F32)
COLUMNS = pltpu.VMEM((ROWS, 2 * HEIGHT, 256), BF16)
BACKS = pltpu.VMEM((ROWS, 2 * HEIGHT, 256), F32)
SQUARE = pltpu.VMEM((256, 256), F32)
WEIGHT = pltpu.VMEM((2, 256, 256), BF16)
POINTS = array((ROWS, 4 * HEIGHT, 256))
PARAMS = pltpu.CompilerParams(vmem_limit_bytes=48 * 1024 * 1024)


def call(kernel, out_shape, scratch, name):
    return pl.pallas_call(kernel, out_shape=out_shape, scratch_shapes=scratch, name=name, compiler_params=PARAMS)


def exchange(value, axis):
    return lax.all_to_all(value, axis, split_axis=0, concat_axis=0, tiled=True)


def to_lat(wire, table):
    field = exchange(wire, "lon").reshape(WIDTH, LANES)
    wire = call(width_kernel, LAT_WIRE, [PEERS], "width")(field, table)
    return exchange(wire, "lat")


def to_lon(wire, table):
    wire = exchange(wire, "lat")
    field = call(
        width_back_kernel, array((WIDTH, LANES)), [PEERS, pltpu.VMEM((WIDTH, LANES), BF16)], "width_back"
    )(wire, table)
    return exchange(field.reshape(LON_WIRE.shape), "lon")


def shards(
    state, spec_weight1, spec_bias1, spec_weight2, spec_bias2, norm1_gain, norm1_bias, norm2_gain, norm2_bias,
    fc1_weight, fc1_bias, fc2_weight, fc2_bias, cotangent,
):
    width_forward, width_inverse = (jnp.asarray(split_table(t)) for t in width_tables())
    height_forward, height_inverse = (
        jnp.asarray(np.stack([split_table(v) for v in t])) for t in height_tables()
    )
    tokens = state.reshape(TOKENS, FEATURES)
    cot = cotangent.reshape(TOKENS, FEATURES)
    gain1, shift1 = norm1_gain.reshape(1, -1), norm1_bias.reshape(1, -1)
    gain2, shift2 = norm2_gain.reshape(1, -1), norm2_bias.reshape(1, -1)
    weight1, weight2 = spec_weight1.reshape(2, BLOCK, BLOCK), spec_weight2.reshape(2, BLOCK, BLOCK)
    bias1, bias2 = spec_bias1.reshape(2, BLOCK), spec_bias2.reshape(2, BLOCK)

    token_array = array((TOKENS, FEATURES))
    lowered, wire = call(begin_kernel, (token_array, LON_WIRE), [BLOCKS], "begin")(tokens, gain1, shift1)
    wire = to_lat(wire, width_forward)
    bias = pltpu.VMEM((1, 256), F32)
    wire, slopes, squares = call(
        filter_kernel,
        (LAT_WIRE, POINTS, POINTS),
        [PEERS, COLUMNS, BACKS, SQUARE, WEIGHT, WEIGHT, bias, bias],
        "filter",
    )(wire, height_forward, height_inverse, weight1, bias1, weight2, bias2)
    wire = to_lon(wire, width_inverse)

    whole = lambda *shape: pl.BlockSpec(shape, lambda i: (0,) * len(shape))
    token_spec = whole(TOKENS, FEATURES)
    wire_spec = whole(*LON_WIRE.shape)
    advanced, grad_mixed, wire = pl.pallas_call(
        token_kernel,
        grid=(HIDDEN // CHUNK,),
        in_specs=[
            wire_spec,
            token_spec,
            token_spec,
            token_spec,
            whole(1, FEATURES),
            whole(1, FEATURES),
            pl.BlockSpec((FEATURES, CHUNK), lambda i: (0, i)),
            pl.BlockSpec((1, CHUNK), lambda i: (0, i)),
            pl.BlockSpec((CHUNK, FEATURES), lambda i: (i, 0)),
            whole(1, FEATURES),
        ],
        out_specs=(token_spec, token_spec, wire_spec),
        out_shape=(token_array, token_array, LON_WIRE),
        scratch_shapes=[
            BLOCKS,
            pltpu.VMEM((TOKENS, FEATURES), BF16),
            pltpu.VMEM((TOKENS, FEATURES), BF16),
            pltpu.VMEM((TOKENS, FEATURES), F32),
            pltpu.VMEM((TOKENS, FEATURES), F32),
        ],
        name="token",
        compiler_params=PARAMS,
    )(
        wire, tokens, lowered, cot, gain2, shift2,
        fc1_weight, fc1_bias.reshape(1, -1), fc2_weight, fc2_bias.reshape(1, -1),
    )

    wire = to_lat(wire, width_forward)
    wire = call(adjoint_kernel, LAT_WIRE, [PEERS, COLUMNS, BACKS, SQUARE, WEIGHT, WEIGHT], "adjoint")(
        wire, height_forward, height_inverse, weight1, weight2, slopes, squares
    )
    wire = to_lon(wire, width_inverse)
    sensitivity = call(finish_kernel, token_array, [BLOCKS], "finish")(wire, grad_mixed, tokens, gain1)
    return advanced.reshape(state.shape), sensitivity.reshape(state.shape)


def solution(mesh):
    field = P("ens", "lat", "lon", None)
    block, bias = P(None, "lon", None, None), P(None, "lon", None)
    return jax.shard_map(
        shards,
        mesh=mesh,
        in_specs=(field, block, bias, block, bias, *[P()] * 8, field),
        out_specs=(field, field),
        check_vma=False,
    )
```

```python
import math

import jax
import jax.numpy as jnp
import numpy as np
from jax import lax
from jax.experimental import pallas as pl
from jax.experimental.pallas import tpu as pltpu
from jax.sharding import PartitionSpec as P

EPSILON = 1e-06
THRESHOLD = 0.01
LATS, LONS = 16, 8
HEIGHT, WIDTH, FEATURES, HIDDEN = 96, 192, 768, 3072
ROWS, COLS = HEIGHT // LATS, WIDTH // LONS
BLOCK = FEATURES // LONS
STATES = 2
GROUPS = STATES * ROWS
TOKENS = GROUPS * COLS
LANES = GROUPS * BLOCK
TILES = LANES // 128
WIRE = TILES * GROUPS
STRIDE = 109
CHUNK = 512
CHUNKS = HIDDEN // CHUNK
UNROLL = 2
F32, BF16 = jnp.float32, jnp.bfloat16


def split_table(table):
    high = table.astype(BF16)
    return np.stack([high, (table - high.astype(np.float64)).astype(BF16)])


def width_tables():
    part, q, d = np.meshgrid(np.arange(2), np.arange(ROWS), np.arange(LATS), indexing="ij")
    part, freq = part.reshape(-1, 1), (q + ROWS * d).reshape(-1, 1)
    w = np.arange(WIDTH).reshape(1, -1)
    angle = 2.0 * math.pi * (freq * w % WIDTH) / WIDTH
    parity = np.where(w % 2 == 0, 1.0, -1.0)
    scale = 1.0 / math.sqrt(WIDTH)
    forward = np.where(part == 0, np.cos(angle), np.where(freq == 0, parity, -np.sin(angle)))
    twice = np.where(freq == 0, 1.0, 2.0)
    return split_table(forward * scale), split_table((forward * twice * scale).T)


def height_tables():
    p = np.arange(HEIGHT).reshape(-1, 1, 1)
    r = np.arange(ROWS).reshape(1, -1, 1)
    s = np.arange(LATS).reshape(1, 1, -1)
    angle = 2.0 * math.pi * (p * (ROWS * s + r) % HEIGHT) / HEIGHT
    c, n = np.cos(angle) / math.sqrt(HEIGHT), np.sin(angle) / math.sqrt(HEIGHT)
    zero = np.zeros_like(c)

    def join(rows):
        return np.concatenate([np.stack(row, axis=2).reshape(HEIGHT, -1) for row in rows], axis=0)

    plain = join([[c, n], [c, n], [-n, c], [n, -c]])
    packed = join([[c, zero], [zero, c], [-n, zero], [zero, -n]])

    def join_back(rows):
        return np.concatenate(
            [np.concatenate([v.reshape(HEIGHT, -1).T for v in row], axis=1) for row in rows], axis=0
        )

    h = 0.5
    plain_back = join_back([[h * c, h * c, -h * n, h * n], [h * n, h * n, h * c, -h * c]])
    packed_back = join_back([[c, zero, -n, zero], [zero, c, zero, -n]])
    return tuple(np.stack([split_table(t) for t in pair]) for pair in ((plain, packed), (plain_back, packed_back)))


def dot(a, b):
    return lax.dot_general(a, b, (((1,), (0,)), ((), ())), preferred_element_type=F32)


def dot_t(a, b):
    return lax.dot_general(a, b, (((1,), (1,)), ((), ())), preferred_element_type=F32)


def lane_index(rows):
    return lax.broadcasted_iota(jnp.int32, (rows, 128), 1)


def unpack4(t0, t1, t2):
    lane = lane_index(t0.shape[0])
    b1 = jnp.where(lane < 32, pltpu.roll(t0, 32, 1), pltpu.roll(t1, 32, 1))
    b2 = jnp.where(lane < 64, pltpu.roll(t1, 64, 1), pltpu.roll(t2, 64, 1))
    return t0, b1, b2, pltpu.roll(t2, 96, 1)


def pack4(b0, b1, b2, b3):
    lane = lane_index(b0.shape[0])
    r1, r2, r3 = pltpu.roll(b1, 96, 1), pltpu.roll(b2, 64, 1), pltpu.roll(b3, 32, 1)
    return (
        jnp.where(lane < 96, b0, r1),
        jnp.where(lane < 64, r1, r2),
        jnp.where(lane < 32, r2, r3),
    )


def row(vector):
    return vector[...].reshape(1, -1)


def norm(values):
    average = jnp.mean(values, axis=-1, keepdims=True)
    centred = values - average
    inverse = lax.rsqrt(jnp.mean(centred * centred, axis=-1, keepdims=True) + EPSILON)
    return centred * inverse, inverse


def norm_backward(gradient, gain, normed, inverse):
    scaled = gradient * gain
    return inverse * (
        scaled
        - jnp.mean(scaled, axis=-1, keepdims=True)
        - normed * jnp.mean(scaled * normed, axis=-1, keepdims=True)
    )


def gelu_pair(values):
    cumulative = 0.5 * (1.0 + lax.erf(values * 0.7071067811865476))
    density = jnp.exp(-0.5 * values * values) * 0.3989422804014327
    return values * cumulative, cumulative + values * density


def scatter_blocks(blocks, pair, values):
    tiles = [values[:, 128 * i : 128 * i + 128] for i in range(6)]
    for j, b in enumerate((*unpack4(*tiles[:3]), *unpack4(*tiles[3:]))):
        blocks[j, 2 * pair] = b[:COLS]
        blocks[j, 2 * pair + 1] = b[COLS:]


def send_blocks(blocks, wire):
    for j in range(LONS):
        for g in range(GROUPS // 4):
            tiles = pack4(*(blocks[j, 4 * g + n] for n in range(4)))
            for i, t in enumerate(tiles):
                at = 384 * g + 128 * i
                wire[j, :, at : at + 128] = t.astype(BF16)


def receive_blocks(wire, blocks):
    for j in range(LONS):
        for g in range(GROUPS // 4):
            at = 384 * g
            tiles = [wire[j, :, at + 128 * i : at + 128 * i + 128].astype(F32) for i in range(3)]
            for n, b in enumerate(unpack4(*tiles)):
                blocks[j, 4 * g + n] = b


def gather_blocks(blocks, pair):
    parts = [jnp.concatenate([blocks[j, 2 * pair], blocks[j, 2 * pair + 1]], axis=0) for j in range(LONS)]
    return jnp.concatenate([*pack4(*parts[:4]), *pack4(*parts[4:])], axis=1)


def fetch(sem, *pairs):
    copies = [pltpu.make_async_copy(source, target, sem.at[n]) for n, (source, target) in enumerate(pairs)]
    for c in copies:
        c.start()

    def wait(*numbers):
        for n in numbers:
            copies[n].wait()

    return wait


def begin_kernel(states, gains, shifts, lowereds, wire, state, gain, shift, lowered, blocks, sem):
    wait = fetch(sem, (states, state), (gains, gain), (shifts, shift))
    wait(0, 1, 2)
    gain, shift = row(gain), row(shift)
    for pair in range(GROUPS // 2):
        rows = slice(48 * pair, 48 * pair + 48)
        normed, _ = norm(state[rows, :].astype(F32))
        value = (normed * gain + shift).astype(BF16)
        lowered[rows, :] = value
        scatter_blocks(blocks, pair, value.astype(F32))
    keep = fetch(sem, (lowered, lowereds))
    send_blocks(blocks, wire)
    keep(0)


def wire_out(scratch, wire):
    for d in range(LATS):
        wire[d] = scratch[STRIDE * d : STRIDE * d + WIRE, :].astype(BF16)


def wire_in(wire, scratch):
    for d in range(LATS):
        scratch[STRIDE * d : STRIDE * d + WIRE, :] = wire[d].astype(F32)


def peers(row):
    return pl.ds(row, LATS, stride=STRIDE)


def width_kernel(field, tables, wire, scratch, table, sem):
    fetch(sem, (tables, table))(0)
    product = dot(table[0], field[...]) + dot(table[1], field[...])
    for e in range(GROUPS):
        for i in range(TILES):
            scratch[peers(GROUPS * i + e), :] = product[16 * e : 16 * e + 16, 128 * i : 128 * i + 128]
    wire_out(scratch, wire)


def width_back_kernel(wire, tables, field, scratch, gathered, table, sem):
    wait = fetch(sem, (tables, table))
    wire_in(wire, scratch)
    for e in range(GROUPS):
        for i in range(TILES):
            piece = scratch[peers(GROUPS * i + e), :]
            gathered[16 * e : 16 * e + 16, 128 * i : 128 * i + 128] = piece.astype(BF16)
    wait(0)
    field[...] = (dot(table[0], gathered[...]) + dot(table[1], gathered[...])).astype(BF16)


def spectrum_in(wire, scratch, columns):
    wire_in(wire, scratch)
    for part in range(2):
        for q in range(ROWS):
            e = ROWS * part + q
            for g in range(GROUPS // 4):
                tiles = [scratch[peers(GROUPS * (3 * g + i) + e), :] for i in range(3)]
                for n, b in enumerate(unpack4(*tiles)):
                    state, r = divmod(4 * g + n, ROWS)
                    at = 16 * (2 * r + part)
                    columns[q, at : at + 16, 128 * state : 128 * state + 128] = b.astype(BF16)


def spectrum_out(backs, scratch, wire):
    for part in range(2):
        for q in range(ROWS):
            e = ROWS * part + q
            for g in range(GROUPS // 4):
                blocks = []
                for n in range(4):
                    state, r = divmod(4 * g + n, ROWS)
                    at = 16 * (ROWS * part + r)
                    blocks.append(backs[q, at : at + 16, 128 * state : 128 * state + 128])
                for i, t in enumerate(pack4(*blocks)):
                    scratch[peers(GROUPS * (3 * g + i) + e), :] = t
    wire_out(scratch, wire)


def build_weight(weight, square, out):
    square[...] = jnp.zeros_like(square)
    square[0:BLOCK, 0:BLOCK] = weight[0]
    square[0:BLOCK, 128 : 128 + BLOCK] = weight[1]
    square[128 : 128 + BLOCK, 0:BLOCK] = -weight[1]
    square[128 : 128 + BLOCK, 128 : 128 + BLOCK] = weight[0]
    full = square[...]
    high = full.astype(BF16)
    out[0] = high
    out[1] = (full - high.astype(F32)).astype(BF16)


def build_bias(bias, out):
    out[...] = jnp.zeros_like(out)
    out[0:1, 0:BLOCK] = bias[0:1, :]
    out[0:1, 128 : 128 + BLOCK] = bias[1:2, :]


def to_points(spectrum):
    half = 2 * HEIGHT
    return jnp.concatenate(
        [
            jnp.concatenate([spectrum[:half, at : at + 128], spectrum[half:, at : at + 128]], axis=1)
            for at in (0, 128)
        ],
        axis=0,
    )


def from_points(points):
    half = 2 * HEIGHT
    return jnp.concatenate(
        [
            jnp.concatenate([points[at : at + half, :128], points[at : at + half, 128:]], axis=0)
            for at in (0, half)
        ],
        axis=1,
    )


def is_packed(q):
    return jnp.where((q == 0) & (lax.axis_index("lat") == 0), 1, 0)


def filter_kernel(
    wire, forwards, inverses, weight1s, bias1s, weight2s, bias2s,
    wire_back, slopes_out, squares_out,
    forward, inverse, weight1, bias1, weight2, bias2, slopes, squares,
    scratch, columns, backs, square, w1, w2, c1, c2, sem, sem_out,
):
    wait = fetch(
        sem, (weight1s, weight1), (bias1s, bias1), (weight2s, weight2), (bias2s, bias2),
        (forwards, forward), (inverses, inverse),
    )
    spectrum_in(wire, scratch, columns)
    wait(0, 1, 2, 3)
    build_weight(weight1, square, w1)
    build_weight(weight2, square, w2)
    build_bias(bias1, c1)
    build_bias(bias2, c2)
    wait(4, 5)

    @pl.loop(0, ROWS, unroll=UNROLL)
    def _(q):
        which = is_packed(q)
        field = columns[q]
        spectrum = dot(forward[which, 0], field) + dot(forward[which, 1], field)
        points = to_points(spectrum.astype(BF16))
        pre = dot(points, w1[0]) + dot(points, w1[1]) + c1[...]
        active, slope = gelu_pair(pre)
        slopes[q] = slope.astype(BF16)
        active = active.astype(BF16)
        post = dot(active, w2[0]) + dot(active, w2[1]) + c2[...]
        bend = jnp.tanh(post * (1.0 / THRESHOLD))
        squares[q] = (bend * bend).astype(BF16)
        shrunk = from_points((post - THRESHOLD * bend).astype(BF16))
        backs[q] = dot(inverse[which, 0], shrunk) + dot(inverse[which, 1], shrunk)

    keep = fetch(sem_out, (slopes, slopes_out), (squares, squares_out))
    spectrum_out(backs, scratch, wire_back)
    keep(0, 1)


def adjoint_kernel(
    wire, forwards, inverses, weight1s, weight2s, slopes_in, squares_in,
    wire_back,
    forward, inverse, weight1, weight2, slopes, squares,
    scratch, columns, backs, square, w1, w2, sem,
):
    wait = fetch(
        sem, (weight1s, weight1), (weight2s, weight2), (forwards, forward), (inverses, inverse),
        (slopes_in, slopes), (squares_in, squares),
    )
    spectrum_in(wire, scratch, columns)
    wait(0, 1)
    build_weight(weight1, square, w1)
    build_weight(weight2, square, w2)
    wait(2, 3, 4, 5)

    @pl.loop(0, ROWS, unroll=UNROLL)
    def _(q):
        which = is_packed(q)
        field = columns[q]
        spectrum = dot(forward[which, 0], field) + dot(forward[which, 1], field)
        points = (to_points(spectrum) * squares[q].astype(F32)).astype(BF16)
        active = dot_t(points, w2[0]) + dot_t(points, w2[1])
        pre = (active * slopes[q].astype(F32)).astype(BF16)
        result = dot_t(pre, w1[0]) + dot_t(pre, w1[1])
        shrunk = from_points(result.astype(BF16))
        backs[q] = dot(inverse[which, 0], shrunk) + dot(inverse[which, 1], shrunk)

    spectrum_out(backs, scratch, wire_back)


def pieces(n):
    return pl.ds(CHUNK * n if isinstance(n, int) else pl.multiple_of(CHUNK * n, CHUNK), CHUNK)


def chunk_copies(sem, copy):
    one = lambda n: pltpu.make_async_copy(*copy(pieces(n)), sem.at[n])
    return lambda n: one(n).start(), lambda n: one(n).wait()


def gradient_kernel(cotangents, fc2s, grad_hiddens, cotangent, fc2, grad_hidden, sem, sem_in, sem_out):
    wait = fetch(sem, (cotangents, cotangent))
    start_in, wait_in = chunk_copies(sem_in, lambda c: (fc2s.at[c, :], fc2.at[c, :]))
    start_out, wait_out = chunk_copies(sem_out, lambda c: (grad_hidden.at[:, c], grad_hiddens.at[:, c]))
    pl.loop(0, CHUNKS)(start_in)
    wait(0)

    @pl.loop(0, CHUNKS)
    def _(n):
        wait_in(n)
        grad_hidden[:, pieces(n)] = dot_t(cotangent[...], fc2[pieces(n), :])
        start_out(n)

    pl.loop(0, CHUNKS)(wait_out)


def token_kernel(
    wire, states, lowereds, cotangents, gains, shifts, fc1s, bias1s, grad_hiddens,
    hiddens, mixeds, grad_mixeds, wire_next,
    state, lowered, cotangent, gain, shift, fc1, bias1, grad_hidden, hidden, mixed, grad_mixed,
    blocks, rows_in, grad_total, sem, sem_fc1, sem_grad, sem_hidden,
):
    wait = fetch(
        sem, (states, state), (lowereds, lowered), (gains, gain), (shifts, shift), (bias1s, bias1),
        (cotangents, cotangent),
    )
    start_fc1, wait_fc1 = chunk_copies(sem_fc1, lambda c: (fc1s.at[:, c], fc1.at[:, c]))
    start_grad, wait_grad = chunk_copies(sem_grad, lambda c: (grad_hiddens.at[:, c], grad_hidden.at[:, c]))
    start_hidden, wait_hidden = chunk_copies(sem_hidden, lambda c: (hidden.at[:, c], hiddens.at[:, c]))

    @pl.loop(0, CHUNKS)
    def _(n):
        start_fc1(n)
        start_grad(n)

    receive_blocks(wire, blocks)
    wait(0, 1, 2, 3, 4)
    for pair in range(GROUPS // 2):
        rows = slice(48 * pair, 48 * pair + 48)
        value = gather_blocks(blocks, pair)
        value = value + lowered[rows, :].astype(F32) + state[rows, :].astype(F32)
        value = value.astype(BF16)
        mixed[rows, :] = value
        normed, _ = norm(value.astype(F32))
        rows_in[rows, :] = (normed * row(gain) + row(shift)).astype(BF16)
    grad_total[...] = jnp.zeros_like(grad_total)

    @pl.loop(0, CHUNKS, unroll=UNROLL)
    def _(n):
        wait_fc1(n)
        hidden_pre = dot(rows_in[...], fc1[:, pieces(n)]) + bias1[:, pieces(n)]
        value, slope = gelu_pair(hidden_pre)
        hidden[:, pieces(n)] = value.astype(BF16)
        start_hidden(n)
        wait_grad(n)
        grad_pre = (grad_hidden[:, pieces(n)] * slope).astype(BF16)
        grad_total[...] += dot_t(grad_pre, fc1[:, pieces(n)])

    wait(5)
    for pair in range(GROUPS // 2):
        rows = slice(48 * pair, 48 * pair + 48)
        normed, scale = norm(mixed[rows, :].astype(F32))
        grad = cotangent[rows, :].astype(F32) + norm_backward(grad_total[rows, :], row(gain), normed, scale)
        grad = grad.astype(BF16)
        grad_mixed[rows, :] = grad
        scatter_blocks(blocks, pair, grad.astype(F32))
    keep = fetch(sem, (mixed, mixeds), (grad_mixed, grad_mixeds))
    send_blocks(blocks, wire_next)
    pl.loop(0, CHUNKS)(wait_hidden)
    keep(0, 1)


def advance_kernel(
    hiddens, fc2s, bias2s, mixeds, advanced, hidden, fc2, bias2, mixed, total, sem, sem_hidden, sem_fc2
):
    wait = fetch(sem, (bias2s, bias2), (mixeds, mixed))
    start_hidden, wait_hidden = chunk_copies(sem_hidden, lambda c: (hiddens.at[:, c], hidden.at[:, c]))
    start_fc2, wait_fc2 = chunk_copies(sem_fc2, lambda c: (fc2s.at[c, :], fc2.at[c, :]))

    @pl.loop(0, CHUNKS)
    def _(n):
        start_hidden(n)
        start_fc2(n)

    wait(0, 1)
    total[...] = mixed[...].astype(F32) + row(bias2)

    @pl.loop(0, CHUNKS)
    def _(n):
        wait_hidden(n)
        wait_fc2(n)
        total[...] += dot(hidden[:, pieces(n)], fc2[pieces(n), :])

    advanced[...] = total[...].astype(BF16)


def finish_kernel(wire, grad_mixeds, states, gains, sensitivity, grad_mixed, state, gain, blocks, sem):
    wait = fetch(sem, (grad_mixeds, grad_mixed), (states, state), (gains, gain))
    receive_blocks(wire, blocks)
    wait(0, 1, 2)
    for pair in range(GROUPS // 2):
        rows = slice(48 * pair, 48 * pair + 48)
        grad = grad_mixed[rows, :].astype(F32)
        normed, scale = norm(state[rows, :].astype(F32))
        grad_lowered = gather_blocks(blocks, pair) + grad
        sensitivity[rows, :] = (grad + norm_backward(grad_lowered, row(gain), normed, scale)).astype(BF16)


def near(*shape, dtype=BF16):
    return jax.ShapeDtypeStruct(shape, dtype)


def vmem(*shape, dtype=BF16):
    return pltpu.VMEM(shape, dtype)


def sems(n):
    return pltpu.SemaphoreType.DMA((n,))


LON_WIRE = near(LONS, COLS, LANES)
LAT_WIRE = near(LATS, WIRE, 128)
BLOCKS = vmem(LONS, GROUPS, COLS, 128, dtype=F32)
PEERS = vmem(LATS * STRIDE, 128, dtype=F32)
WIDTH_TABLE = vmem(2, WIDTH, WIDTH)
HEIGHT_TABLES = (vmem(2, 2, 4 * HEIGHT, 2 * HEIGHT), vmem(2, 2, 2 * HEIGHT, 4 * HEIGHT))
WEIGHT, BIAS = vmem(2, BLOCK, BLOCK, dtype=F32), vmem(2, BLOCK, dtype=F32)
POINTS = (ROWS, 4 * HEIGHT, 256)
SPECTRAL = (
    PEERS,
    vmem(ROWS, 2 * HEIGHT, 256),
    vmem(ROWS, 2 * HEIGHT, 256, dtype=F32),
    vmem(256, 256, dtype=F32),
    vmem(2, 256, 256),
    vmem(2, 256, 256),
)
WIDE_BIAS = vmem(1, 256, dtype=F32)
TOKEN, UNITS = (TOKENS, FEATURES), (TOKENS, HIDDEN)
VECTOR = vmem(FEATURES, dtype=F32)
PARAMS = pltpu.CompilerParams(vmem_limit_bytes=48 * 1024 * 1024)
NEAR, FAR = pl.BlockSpec(), pl.BlockSpec(memory_space=pltpu.HBM)


def far(value):
    return pltpu.with_memory_space_constraint(value, pltpu.HBM)


def call(kernel, out_shape, scratch, near_operands, far_operands, flops=0):
    single = not isinstance(out_shape, tuple)
    shapes = (out_shape,) if single else out_shape
    specs = tuple(NEAR if isinstance(o, jax.ShapeDtypeStruct) else FAR for o in shapes)
    return pl.pallas_call(
        kernel,
        out_shape=out_shape,
        in_specs=[NEAR] * len(near_operands) + [FAR] * len(far_operands),
        out_specs=specs[0] if single else specs,
        scratch_shapes=scratch,
        name=kernel.__name__,
        compiler_params=PARAMS,
        cost_estimate=pl.CostEstimate(flops=flops, bytes_accessed=0, transcendentals=0),
    )(*near_operands, *map(far, far_operands))


def exchange(value, axis):
    return lax.all_to_all(value, axis, split_axis=0, concat_axis=0, tiled=True)


def to_lat(wire, table):
    field = exchange(wire, "lon").reshape(WIDTH, LANES)
    return exchange(call(width_kernel, LAT_WIRE, [PEERS, WIDTH_TABLE, sems(1)], [field], [table]), "lat")


def to_lon(wire, table):
    scratch = [PEERS, vmem(WIDTH, LANES), WIDTH_TABLE, sems(1)]
    field = call(width_back_kernel, near(WIDTH, LANES), scratch, [exchange(wire, "lat")], [table])
    return exchange(field.reshape(LON_WIRE.shape), "lon")


def shards(
    state, spec_weight1, spec_bias1, spec_weight2, spec_bias2, norm1_gain, norm1_bias, norm2_gain, norm2_bias,
    fc1_weight, fc1_bias, fc2_weight, fc2_bias, cotangent,
):
    width_forward, width_inverse = map(jnp.asarray, width_tables())
    height_forward, height_inverse = map(jnp.asarray, height_tables())
    tokens = state.reshape(TOKEN)
    cot = cotangent.reshape(TOKEN)
    weight1, weight2 = spec_weight1.reshape(2, BLOCK, BLOCK), spec_weight2.reshape(2, BLOCK, BLOCK)
    bias1, bias2 = spec_bias1.reshape(2, BLOCK), spec_bias2.reshape(2, BLOCK)
    matmul = 2 * TOKENS * FEATURES * HIDDEN

    lowered, wire = call(
        begin_kernel,
        (pltpu.HBM(TOKEN, BF16), LON_WIRE),
        [vmem(*TOKEN), VECTOR, VECTOR, vmem(*TOKEN), BLOCKS, sems(3)],
        [],
        [tokens, norm1_gain, norm1_bias],
    )
    wire = to_lat(wire, width_forward)
    grad_hidden = call(
        gradient_kernel,
        pltpu.HBM(UNITS, F32),
        [vmem(*TOKEN), vmem(HIDDEN, FEATURES), vmem(*UNITS, dtype=F32), sems(1), sems(CHUNKS), sems(CHUNKS)],
        [],
        [cot, fc2_weight],
        matmul,
    )
    wire, slopes, squares = call(
        filter_kernel,
        (LAT_WIRE, pltpu.HBM(POINTS, BF16), pltpu.HBM(POINTS, BF16)),
        [*HEIGHT_TABLES, WEIGHT, BIAS, WEIGHT, BIAS, vmem(*POINTS), vmem(*POINTS)]
        + [*SPECTRAL, WIDE_BIAS, WIDE_BIAS, sems(6), sems(2)],
        [wire],
        [height_forward, height_inverse, weight1, bias1, weight2, bias2],
    )
    wire = to_lon(wire, width_inverse)

    hidden, mixed, grad_mixed, wire = call(
        token_kernel,
        (pltpu.HBM(UNITS, BF16), pltpu.HBM(TOKEN, BF16), pltpu.HBM(TOKEN, BF16), LON_WIRE),
        [vmem(*TOKEN), vmem(*TOKEN), vmem(*TOKEN), VECTOR, VECTOR, vmem(FEATURES, HIDDEN)]
        + [vmem(1, HIDDEN, dtype=F32), vmem(*UNITS, dtype=F32), vmem(*UNITS), vmem(*TOKEN), vmem(*TOKEN)]
        + [BLOCKS, vmem(*TOKEN), vmem(*TOKEN, dtype=F32), sems(6), sems(CHUNKS), sems(CHUNKS), sems(CHUNKS)],
        [wire],
        [tokens, lowered, cot, norm2_gain, norm2_bias, fc1_weight, fc1_bias.reshape(1, -1), grad_hidden],
        2 * matmul,
    )

    wire = to_lat(wire, width_forward)
    advanced = call(
        advance_kernel,
        near(*TOKEN),
        [vmem(*UNITS), vmem(HIDDEN, FEATURES), VECTOR, vmem(*TOKEN), vmem(*TOKEN, dtype=F32)]
        + [sems(2), sems(CHUNKS), sems(CHUNKS)],
        [],
        [hidden, fc2_weight, fc2_bias, mixed],
        matmul,
    )
    wire = call(
        adjoint_kernel,
        LAT_WIRE,
        [*HEIGHT_TABLES, WEIGHT, WEIGHT, vmem(*POINTS), vmem(*POINTS), *SPECTRAL, sems(6)],
        [wire],
        [height_forward, height_inverse, weight1, weight2, slopes, squares],
    )
    wire = to_lon(wire, width_inverse)
    sensitivity = call(
        finish_kernel,
        near(*TOKEN),
        [vmem(*TOKEN), vmem(*TOKEN), VECTOR, BLOCKS, sems(3)],
        [wire],
        [grad_mixed, tokens, norm1_gain],
    )
    return advanced.reshape(state.shape), sensitivity.reshape(state.shape)


def solution(mesh):
    field = P("ens", "lat", "lon", None)
    block, bias = P(None, "lon", None, None), P(None, "lon", None)
    return jax.shard_map(
        shards,
        mesh=mesh,
        in_specs=(field, block, bias, block, bias, *[P()] * 8, field),
        out_specs=(field, field),
        check_vma=False,
    )
```

```python
import math

import jax
import jax.numpy as jnp
import numpy as np
from jax import lax
from jax.experimental import pallas as pl
from jax.experimental.pallas import tpu as pltpu
from jax.sharding import PartitionSpec as P

EPSILON = 1e-06
THRESHOLD = 0.01
LATS, LONS = 16, 8
HEIGHT, WIDTH, FEATURES, HIDDEN = 96, 192, 768, 3072
ROWS, COLS = HEIGHT // LATS, WIDTH // LONS
BLOCK = FEATURES // LONS
STATES = 2
GROUPS = STATES * ROWS
TOKENS = GROUPS * COLS
LANES = GROUPS * BLOCK
TILES = LANES // 128
WIRE = TILES * GROUPS
STRIDE = 109
CHUNK = 512
CHUNKS = HIDDEN // CHUNK
UNROLL = 2
F32, BF16 = jnp.float32, jnp.bfloat16


def split_table(table):
    high = table.astype(BF16)
    return np.stack([high, (table - high.astype(np.float64)).astype(BF16)])


def width_tables():
    part, q, d = np.meshgrid(np.arange(2), np.arange(ROWS), np.arange(LATS), indexing="ij")
    part, freq = part.reshape(-1, 1), (q + ROWS * d).reshape(-1, 1)
    w = np.arange(WIDTH).reshape(1, -1)
    angle = 2.0 * math.pi * (freq * w % WIDTH) / WIDTH
    parity = np.where(w % 2 == 0, 1.0, -1.0)
    scale = 1.0 / math.sqrt(WIDTH)
    forward = np.where(part == 0, np.cos(angle), np.where(freq == 0, parity, -np.sin(angle)))
    twice = np.where(freq == 0, 1.0, 2.0)
    return split_table(forward * scale), split_table((forward * twice * scale).T)


def height_tables():
    p = np.arange(HEIGHT).reshape(-1, 1, 1)
    r = np.arange(ROWS).reshape(1, -1, 1)
    s = np.arange(LATS).reshape(1, 1, -1)
    angle = 2.0 * math.pi * (p * (ROWS * s + r) % HEIGHT) / HEIGHT
    c, n = np.cos(angle) / math.sqrt(HEIGHT), np.sin(angle) / math.sqrt(HEIGHT)
    zero = np.zeros_like(c)

    def join(rows):
        return np.concatenate([np.stack(row, axis=2).reshape(HEIGHT, -1) for row in rows], axis=0)

    plain = join([[c, n], [c, n], [-n, c], [n, -c]])
    packed = join([[c, zero], [zero, c], [-n, zero], [zero, -n]])

    def join_back(rows):
        return np.concatenate(
            [np.concatenate([v.reshape(HEIGHT, -1).T for v in row], axis=1) for row in rows], axis=0
        )

    h = 0.5
    plain_back = join_back([[h * c, h * c, -h * n, h * n], [h * n, h * n, h * c, -h * c]])
    packed_back = join_back([[c, zero, -n, zero], [zero, c, zero, -n]])
    return np.stack([plain, packed]).astype(BF16), np.stack([plain_back, packed_back]).astype(BF16)


def dot(a, b):
    return lax.dot_general(a, b, (((1,), (0,)), ((), ())), preferred_element_type=F32)


def dot_t(a, b):
    return lax.dot_general(a, b, (((1,), (1,)), ((), ())), preferred_element_type=F32)


def lane_index(rows):
    return lax.broadcasted_iota(jnp.int32, (rows, 128), 1)


def unpack4(t0, t1, t2):
    lane = lane_index(t0.shape[0])
    b1 = jnp.where(lane < 32, pltpu.roll(t0, 32, 1), pltpu.roll(t1, 32, 1))
    b2 = jnp.where(lane < 64, pltpu.roll(t1, 64, 1), pltpu.roll(t2, 64, 1))
    return t0, b1, b2, pltpu.roll(t2, 96, 1)


def pack4(b0, b1, b2, b3):
    lane = lane_index(b0.shape[0])
    r1, r2, r3 = pltpu.roll(b1, 96, 1), pltpu.roll(b2, 64, 1), pltpu.roll(b3, 32, 1)
    return (
        jnp.where(lane < 96, b0, r1),
        jnp.where(lane < 64, r1, r2),
        jnp.where(lane < 32, r2, r3),
    )


def row(vector):
    return vector[...].reshape(1, -1)


def norm(values):
    average = jnp.mean(values, axis=-1, keepdims=True)
    centred = values - average
    inverse = lax.rsqrt(jnp.mean(centred * centred, axis=-1, keepdims=True) + EPSILON)
    return centred * inverse, inverse


def norm_backward(gradient, gain, normed, inverse):
    scaled = gradient * gain
    return inverse * (
        scaled
        - jnp.mean(scaled, axis=-1, keepdims=True)
        - normed * jnp.mean(scaled * normed, axis=-1, keepdims=True)
    )


def gelu_pair(values):
    cumulative = 0.5 * (1.0 + lax.erf(values * 0.7071067811865476))
    density = jnp.exp(-0.5 * values * values) * 0.3989422804014327
    return values * cumulative, cumulative + values * density


def scatter_blocks(blocks, pair, values):
    tiles = [values[:, 128 * i : 128 * i + 128] for i in range(6)]
    for j, b in enumerate((*unpack4(*tiles[:3]), *unpack4(*tiles[3:]))):
        blocks[j, 2 * pair] = b[:COLS]
        blocks[j, 2 * pair + 1] = b[COLS:]


def send_blocks(blocks, wire):
    for j in range(LONS):
        for g in range(GROUPS // 4):
            tiles = pack4(*(blocks[j, 4 * g + n] for n in range(4)))
            for i, t in enumerate(tiles):
                at = 384 * g + 128 * i
                wire[j, :, at : at + 128] = t.astype(BF16)


def receive_blocks(wire, blocks):
    for j in range(LONS):
        for g in range(GROUPS // 4):
            at = 384 * g
            tiles = [wire[j, :, at + 128 * i : at + 128 * i + 128].astype(F32) for i in range(3)]
            for n, b in enumerate(unpack4(*tiles)):
                blocks[j, 4 * g + n] = b


def gather_blocks(blocks, pair):
    parts = [jnp.concatenate([blocks[j, 2 * pair], blocks[j, 2 * pair + 1]], axis=0) for j in range(LONS)]
    return jnp.concatenate([*pack4(*parts[:4]), *pack4(*parts[4:])], axis=1)


def fetch(sem, *pairs):
    copies = [pltpu.make_async_copy(source, target, sem.at[n]) for n, (source, target) in enumerate(pairs)]
    for c in copies:
        c.start()

    def wait(*numbers):
        for n in numbers:
            copies[n].wait()

    return wait


def pair_rows(pair):
    return slice(48 * pair, 48 * pair + 48)


def begin_kernel(
    states, gains, shifts, *rest
):
    sources, (lowered, wire), targets = rest[:KEPT], rest[KEPT : KEPT + 2], rest[KEPT + 2 : 2 * KEPT + 2]
    state, gain, shift, blocks, sem, sem_kept = rest[2 * KEPT + 2 :]
    vectors = [(gains, gain), (shifts, shift)]
    wait = fetch(sem, *((states.at[pair_rows(n), :], state.at[pair_rows(n), :]) for n in range(GROUPS // 2)), *vectors)
    wait_kept = fetch(sem_kept, *zip(sources, targets))
    wait(6, 7)
    for pair in range(GROUPS // 2):
        rows = pair_rows(pair)
        wait(pair)
        normed, _ = norm(state[rows, :].astype(F32))
        value = (normed * row(gain) + row(shift)).astype(BF16)
        lowered[rows, :] = value
        scatter_blocks(blocks, pair, value.astype(F32))
    send_blocks(blocks, wire)
    wait_kept(*range(KEPT))


def wire_out(scratch, wire):
    for d in range(LATS):
        wire[d] = scratch[STRIDE * d : STRIDE * d + WIRE, :].astype(BF16)


def wire_in(wire, scratch):
    for d in range(LATS):
        scratch[STRIDE * d : STRIDE * d + WIRE, :] = wire[d].astype(F32)


def peers(row):
    return pl.ds(row, LATS, stride=STRIDE)


def width_kernel(field, table, wire, scratch):
    product = dot(table[0], field[...]) + dot(table[1], field[...])
    for e in range(GROUPS):
        for i in range(TILES):
            scratch[peers(GROUPS * i + e), :] = product[16 * e : 16 * e + 16, 128 * i : 128 * i + 128]
    wire_out(scratch, wire)


def width_back_kernel(wire, table, field, scratch, gathered):
    wire_in(wire, scratch)
    for e in range(GROUPS):
        for i in range(TILES):
            piece = scratch[peers(GROUPS * i + e), :]
            gathered[16 * e : 16 * e + 16, 128 * i : 128 * i + 128] = piece.astype(BF16)
    field[...] = (dot(table[0], gathered[...]) + dot(table[1], gathered[...])).astype(BF16)


def spectrum_in(wire, scratch, columns):
    wire_in(wire, scratch)
    for part in range(2):
        for q in range(ROWS):
            e = ROWS * part + q
            for g in range(GROUPS // 4):
                tiles = [scratch[peers(GROUPS * (3 * g + i) + e), :] for i in range(3)]
                for n, b in enumerate(unpack4(*tiles)):
                    state, r = divmod(4 * g + n, ROWS)
                    at = 16 * (2 * r + part)
                    columns[q, at : at + 16, 128 * state : 128 * state + 128] = b.astype(BF16)


def spectrum_out(backs, scratch, wire):
    for part in range(2):
        for q in range(ROWS):
            e = ROWS * part + q
            for g in range(GROUPS // 4):
                blocks = []
                for n in range(4):
                    state, r = divmod(4 * g + n, ROWS)
                    at = 16 * (ROWS * part + r)
                    blocks.append(backs[q, at : at + 16, 128 * state : 128 * state + 128])
                for i, t in enumerate(pack4(*blocks)):
                    scratch[peers(GROUPS * (3 * g + i) + e), :] = t
    wire_out(scratch, wire)


def build_weight(weight, square, out):
    square[...] = jnp.zeros_like(square)
    square[0:BLOCK, 0:BLOCK] = weight[0]
    square[0:BLOCK, 128 : 128 + BLOCK] = weight[1]
    square[128 : 128 + BLOCK, 0:BLOCK] = -weight[1]
    square[128 : 128 + BLOCK, 128 : 128 + BLOCK] = weight[0]
    out[...] = square[...].astype(BF16)


def build_bias(bias, out):
    out[...] = jnp.zeros_like(out)
    out[0:1, 0:BLOCK] = bias[0:1, :]
    out[0:1, 128 : 128 + BLOCK] = bias[1:2, :]


def to_points(spectrum):
    half = 2 * HEIGHT
    return jnp.concatenate(
        [
            jnp.concatenate([spectrum[:half, at : at + 128], spectrum[half:, at : at + 128]], axis=1)
            for at in (0, 128)
        ],
        axis=0,
    )


def from_points(points):
    half = 2 * HEIGHT
    return jnp.concatenate(
        [
            jnp.concatenate([points[at : at + half, :128], points[at : at + half, 128:]], axis=0)
            for at in (0, half)
        ],
        axis=1,
    )


def is_packed(q):
    return jnp.where((q == 0) & (lax.axis_index("lat") == 0), 1, 0)


def filter_kernel(
    wire, forward, inverse, weight1, bias1, weight2, bias2,
    wire_back, slopes_out, squares_out,
    slopes, squares, scratch, columns, backs, square, w1, w2, c1, c2, sem,
):
    build_weight(weight1, square, w1)
    build_weight(weight2, square, w2)
    build_bias(bias1, c1)
    build_bias(bias2, c2)
    spectrum_in(wire, scratch, columns)

    @pl.loop(0, ROWS, unroll=UNROLL)
    def _(q):
        which = is_packed(q)
        points = to_points(dot(forward[which], columns[q]).astype(BF16))
        active, slope = gelu_pair(dot(points, w1[...]) + c1[...])
        slopes[q] = slope.astype(BF16)
        post = dot(active.astype(BF16), w2[...]) + c2[...]
        bend = jnp.tanh(post * (1.0 / THRESHOLD))
        squares[q] = (bend * bend).astype(BF16)
        shrunk = from_points((post - THRESHOLD * bend).astype(BF16))
        backs[q] = dot(inverse[which], shrunk)

    keep = fetch(sem, (slopes, slopes_out), (squares, squares_out))
    spectrum_out(backs, scratch, wire_back)
    keep(0, 1)


def adjoint_kernel(
    wire, forward, inverse, weight1, weight2, slopes, squares,
    wire_back,
    scratch, columns, backs, square, w1, w2,
):
    build_weight(weight1, square, w1)
    build_weight(weight2, square, w2)
    spectrum_in(wire, scratch, columns)

    @pl.loop(0, ROWS, unroll=UNROLL)
    def _(q):
        which = is_packed(q)
        spectrum = dot(forward[which], columns[q])
        points = (to_points(spectrum) * squares[q].astype(F32)).astype(BF16)
        pre = (dot_t(points, w2[...]) * slopes[q].astype(F32)).astype(BF16)
        shrunk = from_points(dot_t(pre, w1[...]).astype(BF16))
        backs[q] = dot(inverse[which], shrunk)

    spectrum_out(backs, scratch, wire_back)


def pieces(n):
    return pl.ds(CHUNK * n if isinstance(n, int) else pl.multiple_of(CHUNK * n, CHUNK), CHUNK)


def chunk_copies(sem, copy):
    one = lambda n: pltpu.make_async_copy(*copy(pieces(n)), sem.at[n])
    return lambda n: one(n).start(), lambda n: one(n).wait()


def gradient_kernel(
    states, lowereds, cotangents, fc2s,
    grad_hiddens, base, cotangent,
    state, lowered, fc2, grad_hidden, sem, sem_in, sem_out,
):
    wait = fetch(sem, (cotangents, cotangent), (states, state), (lowereds, lowered))
    start_in, wait_in = chunk_copies(sem_in, lambda c: (fc2s.at[c, :], fc2.at[c, :]))
    start_out, wait_out = chunk_copies(sem_out, lambda c: (grad_hidden.at[:, c], grad_hiddens.at[:, c]))
    pl.loop(0, CHUNKS)(start_in)
    wait(0)

    @pl.loop(0, CHUNKS)
    def _(n):
        wait_in(n)
        grad_hidden[:, pieces(n)] = dot_t(cotangent[...], fc2[pieces(n), :])
        start_out(n)

    wait(1, 2)
    base[...] = lowered[...].astype(F32) + state[...].astype(F32)
    pl.loop(0, CHUNKS)(wait_out)


def token_kernel(
    wire, base, cotangent, gains, shifts, fc1s, bias1s, grad_hiddens,
    hiddens, mixeds, grad_mixeds, wire_next,
    gain, shift, fc1, bias1, grad_hidden, hidden, mixed, grad_mixed,
    blocks, rows_in, grad_total, sem, sem_fc1, sem_grad, sem_hidden,
):
    wait = fetch(sem, (gains, gain), (shifts, shift), (bias1s, bias1))
    start_fc1, wait_fc1 = chunk_copies(sem_fc1, lambda c: (fc1s.at[:, c], fc1.at[:, c]))
    start_grad, wait_grad = chunk_copies(sem_grad, lambda c: (grad_hiddens.at[:, c], grad_hidden.at[:, c]))
    start_hidden, wait_hidden = chunk_copies(sem_hidden, lambda c: (hidden.at[:, c], hiddens.at[:, c]))

    @pl.loop(0, CHUNKS)
    def _(n):
        start_fc1(n)
        start_grad(n)

    receive_blocks(wire, blocks)
    wait(0, 1, 2)
    for pair in range(GROUPS // 2):
        rows = pair_rows(pair)
        value = (gather_blocks(blocks, pair) + base[rows, :]).astype(BF16)
        mixed[rows, :] = value
        normed, _ = norm(value.astype(F32))
        rows_in[rows, :] = (normed * row(gain) + row(shift)).astype(BF16)
    grad_total[...] = jnp.zeros_like(grad_total)

    @pl.loop(0, CHUNKS, unroll=UNROLL)
    def _(n):
        wait_fc1(n)
        hidden_pre = dot(rows_in[...], fc1[:, pieces(n)]) + bias1[:, pieces(n)]
        value, slope = gelu_pair(hidden_pre)
        hidden[:, pieces(n)] = value.astype(BF16)
        start_hidden(n)
        wait_grad(n)
        grad_pre = (grad_hidden[:, pieces(n)] * slope).astype(BF16)
        grad_total[...] += dot_t(grad_pre, fc1[:, pieces(n)])

    for pair in range(GROUPS // 2):
        rows = pair_rows(pair)
        normed, scale = norm(mixed[rows, :].astype(F32))
        grad = cotangent[rows, :].astype(F32) + norm_backward(grad_total[rows, :], row(gain), normed, scale)
        grad = grad.astype(BF16)
        grad_mixed[rows, :] = grad
        scatter_blocks(blocks, pair, grad.astype(F32))
    keep = fetch(sem, (mixed, mixeds), (grad_mixed, grad_mixeds))
    send_blocks(blocks, wire_next)
    pl.loop(0, CHUNKS)(wait_hidden)
    keep(0, 1)


def advance_kernel(
    hiddens, fc2s, bias2s, mixeds, grad_mixeds, states,
    advanced, normed, scale, grad_mixed,
    hidden, fc2, bias2, mixed, state, total, sem, sem_hidden, sem_fc2,
):
    wait = fetch(sem, (bias2s, bias2), (mixeds, mixed), (grad_mixeds, grad_mixed), (states, state))
    start_hidden, wait_hidden = chunk_copies(sem_hidden, lambda c: (hiddens.at[:, c], hidden.at[:, c]))
    start_fc2, wait_fc2 = chunk_copies(sem_fc2, lambda c: (fc2s.at[c, :], fc2.at[c, :]))

    @pl.loop(0, CHUNKS)
    def _(n):
        start_hidden(n)
        start_fc2(n)

    wait(0, 1, 2, 3)
    for pair in range(GROUPS // 2):
        rows = pair_rows(pair)
        normed[rows, :], scale[rows, :] = norm(state[rows, :].astype(F32))
    total[...] = mixed[...].astype(F32) + row(bias2)

    @pl.loop(0, CHUNKS)
    def _(n):
        wait_hidden(n)
        wait_fc2(n)
        total[...] += dot(hidden[:, pieces(n)], fc2[pieces(n), :])

    advanced[...] = total[...].astype(BF16)


def finish_kernel(wire, normed, scale, grad_mixed, gains, sensitivity, gain, blocks, out, sem, sem_out):
    wait = fetch(sem, (gains, gain))
    receive_blocks(wire, blocks)
    wait(0)
    copies = []
    for pair in range(GROUPS // 2):
        rows = pair_rows(pair)
        grad = grad_mixed[rows, :].astype(F32)
        grad_lowered = gather_blocks(blocks, pair) + grad
        grad = grad + norm_backward(grad_lowered, row(gain), normed[rows, :], scale[rows, :])
        out[rows, :] = grad.astype(BF16)
        copies.append(pltpu.make_async_copy(out.at[rows, :], sensitivity.at[rows, :], sem_out.at[pair]))
        copies[-1].start()
    for c in copies:
        c.wait()


def near(*shape, dtype=BF16):
    return jax.ShapeDtypeStruct(shape, dtype)


def vmem(*shape, dtype=BF16):
    return pltpu.VMEM(shape, dtype)


def sems(n):
    return pltpu.SemaphoreType.DMA((n,))


LON_WIRE = near(LONS, COLS, LANES)
LAT_WIRE = near(LATS, WIRE, 128)
BLOCKS = vmem(LONS, GROUPS, COLS, 128, dtype=F32)
PEERS = vmem(LATS * STRIDE, 128, dtype=F32)
POINTS = (ROWS, 4 * HEIGHT, 256)
SPECTRAL = (
    PEERS,
    vmem(ROWS, 2 * HEIGHT, 256),
    vmem(ROWS, 2 * HEIGHT, 256, dtype=F32),
    vmem(256, 256, dtype=F32),
    vmem(256, 256),
    vmem(256, 256),
)
WIDE_BIAS = vmem(1, 256, dtype=F32)
TOKEN, UNITS = (TOKENS, FEATURES), (TOKENS, HIDDEN)
VECTOR = vmem(FEATURES, dtype=F32)
PARAMS = pltpu.CompilerParams(vmem_limit_bytes=48 * 1024 * 1024)
KEPT = 8


def place(space):
    return pl.BlockSpec() if space is None else pl.BlockSpec(memory_space=space)


def call(kernel, out_shape, scratch, operands, places, flops=0):
    single = not isinstance(out_shape, tuple)
    shapes = (out_shape,) if single else out_shape
    specs = tuple(place(None if isinstance(o, jax.ShapeDtypeStruct) else o.memory_space) for o in shapes)
    spaces = [{"f": pltpu.HBM, "h": pltpu.VMEM, "n": None}[p] for p in places]
    return pl.pallas_call(
        kernel,
        out_shape=out_shape,
        in_specs=[place(m) for m in spaces],
        out_specs=specs[0] if single else specs,
        scratch_shapes=scratch,
        name=kernel.__name__,
        compiler_params=PARAMS,
        cost_estimate=pl.CostEstimate(flops=flops, bytes_accessed=0, transcendentals=0),
    )(*(v if m is None else pltpu.with_memory_space_constraint(v, m) for v, m in zip(operands, spaces, strict=True)))


def exchange(value, axis):
    return lax.all_to_all(value, axis, split_axis=0, concat_axis=0, tiled=True)


def to_lat(wire, table):
    field = exchange(wire, "lon").reshape(WIDTH, LANES)
    return exchange(call(width_kernel, LAT_WIRE, [PEERS], [field, table], "nh"), "lat")


def to_lon(wire, table):
    scratch = [PEERS, vmem(WIDTH, LANES)]
    field = call(width_back_kernel, near(WIDTH, LANES), scratch, [exchange(wire, "lat"), table], "nh")
    return exchange(field.reshape(LON_WIRE.shape), "lon")


def shards(
    state, spec_weight1, spec_bias1, spec_weight2, spec_bias2, norm1_gain, norm1_bias, norm2_gain, norm2_bias,
    fc1_weight, fc1_bias, fc2_weight, fc2_bias, cotangent,
):
    tokens = state.reshape(TOKEN)
    cot = cotangent.reshape(TOKEN)
    matmul = 2 * TOKENS * FEATURES * HIDDEN
    kept = [
        *map(jnp.asarray, (*width_tables(), *height_tables())),
        spec_weight1.reshape(2, BLOCK, BLOCK),
        spec_bias1.reshape(2, BLOCK),
        spec_weight2.reshape(2, BLOCK, BLOCK),
        spec_bias2.reshape(2, BLOCK),
    ]

    lowered, wire, *kept = call(
        begin_kernel,
        (near(*TOKEN), LON_WIRE, *(vmem(*k.shape, dtype=k.dtype) for k in kept)),
        [vmem(*TOKEN), VECTOR, VECTOR, BLOCKS, sems(8), sems(KEPT)],
        [tokens, norm1_gain, norm1_bias, *kept],
        "fff" + "f" * KEPT,
    )
    width_forward, width_inverse, height_forward, height_inverse, weight1, bias1, weight2, bias2 = kept
    wire = to_lat(wire, width_forward)
    wire, slopes, squares = call(
        filter_kernel,
        (LAT_WIRE, pltpu.HBM(POINTS, BF16), pltpu.HBM(POINTS, BF16)),
        [vmem(*POINTS), vmem(*POINTS), *SPECTRAL, WIDE_BIAS, WIDE_BIAS, sems(2)],
        [wire, height_forward, height_inverse, weight1, bias1, weight2, bias2],
        "nhhhhhh",
    )
    grad_hidden, base, cot = call(
        gradient_kernel,
        (pltpu.HBM(UNITS, F32), vmem(*TOKEN, dtype=F32), vmem(*TOKEN)),
        [vmem(*TOKEN), vmem(*TOKEN), vmem(HIDDEN, FEATURES), vmem(*UNITS, dtype=F32)]
        + [sems(3), sems(CHUNKS), sems(CHUNKS)],
        [tokens, lowered, cot, fc2_weight],
        "fnff",
        matmul,
    )
    wire = to_lon(wire, width_inverse)

    hidden, mixed, grad_mixed, wire = call(
        token_kernel,
        (pltpu.HBM(UNITS, BF16), pltpu.HBM(TOKEN, BF16), pltpu.HBM(TOKEN, BF16), LON_WIRE),
        [VECTOR, VECTOR, vmem(FEATURES, HIDDEN), vmem(1, HIDDEN, dtype=F32), vmem(*UNITS, dtype=F32)]
        + [vmem(*UNITS), vmem(*TOKEN), vmem(*TOKEN), BLOCKS, vmem(*TOKEN), vmem(*TOKEN, dtype=F32)]
        + [sems(3), sems(CHUNKS), sems(CHUNKS), sems(CHUNKS)],
        [wire, base, cot, norm2_gain, norm2_bias, fc1_weight, fc1_bias.reshape(1, -1), grad_hidden],
        "nhhfffff",
        2 * matmul,
    )

    wire = to_lat(wire, width_forward)
    wire = call(
        adjoint_kernel,
        LAT_WIRE,
        [*SPECTRAL],
        [wire, height_forward, height_inverse, weight1, weight2, slopes, squares],
        "nhhhhnn",
    )
    advanced, normed, scale, grad_mixed = call(
        advance_kernel,
        (near(*TOKEN), vmem(*TOKEN, dtype=F32), vmem(TOKENS, 1, dtype=F32), vmem(*TOKEN)),
        [vmem(*UNITS), vmem(HIDDEN, FEATURES), VECTOR, vmem(*TOKEN), vmem(*TOKEN), vmem(*TOKEN, dtype=F32)]
        + [sems(4), sems(CHUNKS), sems(CHUNKS)],
        [hidden, fc2_weight, fc2_bias, mixed, grad_mixed, tokens],
        "ffffff",
        matmul,
    )
    wire = to_lon(wire, width_inverse)
    sensitivity = call(
        finish_kernel,
        pltpu.HBM(TOKEN, BF16),
        [VECTOR, BLOCKS, vmem(*TOKEN), sems(1), sems(GROUPS // 2)],
        [wire, normed, scale, grad_mixed, norm1_gain],
        "nhhhf",
    )
    return advanced.reshape(state.shape), sensitivity.reshape(state.shape)


def solution(mesh):
    field = P("ens", "lat", "lon", None)
    block, bias = P(None, "lon", None, None), P(None, "lon", None)
    return jax.shard_map(
        shards,
        mesh=mesh,
        in_specs=(field, block, bias, block, bias, *[P()] * 8, field),
        out_specs=(field, field),
        check_vma=False,
    )
```

```python
import math

import jax
import jax.numpy as jnp
import numpy as np
from jax import lax
from jax.experimental import pallas as pl
from jax.experimental.pallas import tpu as pltpu
from jax.sharding import PartitionSpec as P

EPSILON = 1e-06
THRESHOLD = 0.01
LATS, LONS = 16, 8
HEIGHT, WIDTH, FEATURES, HIDDEN = 96, 192, 768, 3072
ROWS, COLS = HEIGHT // LATS, WIDTH // LONS
BLOCK = FEATURES // LONS
STATES = 2
GROUPS = STATES * ROWS
TOKENS = GROUPS * COLS
LANES = GROUPS * BLOCK
TILES = LANES // 128
WIRE = TILES * GROUPS
STRIDE = 109
CHUNK = 1536
BATCH = 6
BATCHES = GROUPS // BATCH
CHUNKS = HIDDEN // CHUNK
F32, BF16 = jnp.float32, jnp.bfloat16


def split_table(table):
    high = table.astype(BF16)
    return np.stack([high, (table - high.astype(np.float64)).astype(BF16)])


def width_tables():
    part, q, d = np.meshgrid(np.arange(2), np.arange(ROWS), np.arange(LATS), indexing="ij")
    part, freq = part.reshape(-1, 1), (q + ROWS * d).reshape(-1, 1)
    w = np.arange(WIDTH).reshape(1, -1)
    angle = 2.0 * math.pi * (freq * w % WIDTH) / WIDTH
    parity = np.where(w % 2 == 0, 1.0, -1.0)
    scale = 1.0 / math.sqrt(WIDTH)
    forward = np.where(part == 0, np.cos(angle), np.where(freq == 0, parity, -np.sin(angle)))
    twice = np.where(freq == 0, 1.0, 2.0)
    return split_table(forward * scale), split_table((forward * twice * scale).T)


def height_tables():
    p = np.arange(HEIGHT).reshape(-1, 1, 1)
    r = np.arange(ROWS).reshape(1, -1, 1)
    s = np.arange(LATS).reshape(1, 1, -1)
    angle = 2.0 * math.pi * (p * (ROWS * s + r) % HEIGHT) / HEIGHT
    c, n = np.cos(angle) / math.sqrt(HEIGHT), np.sin(angle) / math.sqrt(HEIGHT)
    zero = np.zeros_like(c)

    def join(rows):
        return np.concatenate([np.stack(row, axis=2).reshape(HEIGHT, -1) for row in rows], axis=0)

    plain = join([[c, n], [c, n], [-n, c], [n, -c]])
    packed = join([[c, zero], [zero, c], [-n, zero], [zero, -n]])

    def join_back(rows):
        return np.concatenate(
            [np.concatenate([v.reshape(HEIGHT, -1).T for v in row], axis=1) for row in rows], axis=0
        )

    h = 0.5
    plain_back = join_back([[h * c, h * c, -h * n, h * n], [h * n, h * n, h * c, -h * c]])
    packed_back = join_back([[c, zero, -n, zero], [zero, c, zero, -n]])
    return np.stack([plain, packed]).astype(BF16), np.stack([plain_back, packed_back]).astype(BF16)


def dot(a, b):
    return lax.dot_general(a, b, (((1,), (0,)), ((), ())), preferred_element_type=F32)


def dot_t(a, b):
    return lax.dot_general(a, b, (((1,), (1,)), ((), ())), preferred_element_type=F32)


def lane_index(rows):
    return lax.broadcasted_iota(jnp.int32, (rows, 128), 1)


def unpack4(t0, t1, t2):
    lane = lane_index(t0.shape[0])
    b1 = jnp.where(lane < 32, pltpu.roll(t0, 32, 1), pltpu.roll(t1, 32, 1))
    b2 = jnp.where(lane < 64, pltpu.roll(t1, 64, 1), pltpu.roll(t2, 64, 1))
    return t0, b1, b2, pltpu.roll(t2, 96, 1)


def pack4(b0, b1, b2, b3):
    lane = lane_index(b0.shape[0])
    r1, r2, r3 = pltpu.roll(b1, 96, 1), pltpu.roll(b2, 64, 1), pltpu.roll(b3, 32, 1)
    return (
        jnp.where(lane < 96, b0, r1),
        jnp.where(lane < 64, r1, r2),
        jnp.where(lane < 32, r2, r3),
    )


def row(vector):
    return vector[...].reshape(1, -1)


def norm(values):
    average = jnp.mean(values, axis=-1, keepdims=True)
    centred = values - average
    inverse = lax.rsqrt(jnp.mean(centred * centred, axis=-1, keepdims=True) + EPSILON)
    return centred * inverse, inverse


def norm_backward(gradient, gain, normed, inverse):
    scaled = gradient * gain
    return inverse * (
        scaled
        - jnp.mean(scaled, axis=-1, keepdims=True)
        - normed * jnp.mean(scaled * normed, axis=-1, keepdims=True)
    )


def gelu_pair(values):
    cumulative = 0.5 * (1.0 + lax.erf(values * 0.7071067811865476))
    density = jnp.exp(-0.5 * values * values) * 0.3989422804014327
    return values * cumulative, cumulative + values * density


def scatter_blocks(blocks, batch, values):
    tiles = [values[:, 128 * i : 128 * i + 128] for i in range(6)]
    for j, b in enumerate((*unpack4(*tiles[:3]), *unpack4(*tiles[3:]))):
        for n in range(BATCH):
            blocks[j, BATCH * batch + n] = b[COLS * n : COLS * n + COLS]


def send_blocks(blocks, wire):
    for j in range(LONS):
        for g in range(GROUPS // 4):
            tiles = pack4(*(blocks[j, 4 * g + n] for n in range(4)))
            for i, t in enumerate(tiles):
                at = 384 * g + 128 * i
                wire[j, :, at : at + 128] = t.astype(BF16)


def receive_blocks(wire, blocks):
    for j in range(LONS):
        for g in range(GROUPS // 4):
            at = 384 * g
            tiles = [wire[j, :, at + 128 * i : at + 128 * i + 128].astype(F32) for i in range(3)]
            for n, b in enumerate(unpack4(*tiles)):
                blocks[j, 4 * g + n] = b


def gather_blocks(blocks, batch):
    groups = range(BATCH * batch, BATCH * batch + BATCH)
    parts = [jnp.concatenate([blocks[j, k] for k in groups], axis=0) for j in range(LONS)]
    return jnp.concatenate([*pack4(*parts[:4]), *pack4(*parts[4:])], axis=1)


def fetch(sem, *pairs):
    copies = [pltpu.make_async_copy(source, target, sem.at[n]) for n, (source, target) in enumerate(pairs)]
    for c in copies:
        c.start()

    def wait(*numbers):
        for n in numbers:
            copies[n].wait()

    return wait


def batch_rows(batch):
    size = BATCH * COLS
    return slice(size * batch, size * batch + size)


def begin_kernel(states, gains, shifts, wire, state, gain, shift, blocks, sem):
    fetch(sem, (states, state), (gains, gain), (shifts, shift))(0, 1, 2)
    for batch in range(BATCHES):
        normed, _ = norm(state[batch_rows(batch), :].astype(F32))
        value = (normed * row(gain) + row(shift)).astype(BF16)
        scatter_blocks(blocks, batch, value.astype(F32))
    send_blocks(blocks, wire)


def keep_kernel(*refs):
    sem = refs[-1]
    half = len(refs) // 2
    fetch(sem, *zip(refs[:half], refs[half:-1], strict=True))(*range(half))


def wire_out(scratch, wire):
    for d in range(LATS):
        wire[d] = scratch[STRIDE * d : STRIDE * d + WIRE, :].astype(BF16)


def wire_in(wire, scratch):
    for d in range(LATS):
        scratch[STRIDE * d : STRIDE * d + WIRE, :] = wire[d].astype(F32)


def peers(row):
    return pl.ds(row, LATS, stride=STRIDE)


def width_kernel(field, table, wire, scratch):
    product = dot(table[0], field[...]) + dot(table[1], field[...])
    for e in range(GROUPS):
        for i in range(TILES):
            scratch[peers(GROUPS * i + e), :] = product[16 * e : 16 * e + 16, 128 * i : 128 * i + 128]
    wire_out(scratch, wire)


def width_back_kernel(wire, table, field, scratch, gathered):
    wire_in(wire, scratch)
    for e in range(GROUPS):
        for i in range(TILES):
            piece = scratch[peers(GROUPS * i + e), :]
            gathered[16 * e : 16 * e + 16, 128 * i : 128 * i + 128] = piece.astype(BF16)
    field[...] = (dot(table[0], gathered[...]) + dot(table[1], gathered[...])).astype(BF16)


def spectrum_in(wire, scratch, columns):
    wire_in(wire, scratch)
    for part in range(2):
        for q in range(ROWS):
            e = ROWS * part + q
            for g in range(GROUPS // 4):
                tiles = [scratch[peers(GROUPS * (3 * g + i) + e), :] for i in range(3)]
                for n, b in enumerate(unpack4(*tiles)):
                    state, r = divmod(4 * g + n, ROWS)
                    at = 16 * (2 * r + part)
                    columns[q, at : at + 16, 128 * state : 128 * state + 128] = b.astype(BF16)


def spectrum_out(backs, scratch, wire):
    for part in range(2):
        for q in range(ROWS):
            e = ROWS * part + q
            for g in range(GROUPS // 4):
                blocks = []
                for n in range(4):
                    state, r = divmod(4 * g + n, ROWS)
                    at = 16 * (ROWS * part + r)
                    blocks.append(backs[q, at : at + 16, 128 * state : 128 * state + 128])
                for i, t in enumerate(pack4(*blocks)):
                    scratch[peers(GROUPS * (3 * g + i) + e), :] = t
    wire_out(scratch, wire)


def build_weight(weight, square, out):
    square[...] = jnp.zeros_like(square)
    square[0:BLOCK, 0:BLOCK] = weight[0]
    square[0:BLOCK, 128 : 128 + BLOCK] = weight[1]
    square[128 : 128 + BLOCK, 0:BLOCK] = -weight[1]
    square[128 : 128 + BLOCK, 128 : 128 + BLOCK] = weight[0]
    out[...] = square[...].astype(BF16)


def build_bias(bias, out):
    out[...] = jnp.zeros_like(out)
    out[0:1, 0:BLOCK] = bias[0:1, :]
    out[0:1, 128 : 128 + BLOCK] = bias[1:2, :]


def to_points(spectrum):
    half = 2 * HEIGHT
    return jnp.concatenate(
        [
            jnp.concatenate([spectrum[:half, at : at + 128], spectrum[half:, at : at + 128]], axis=1)
            for at in (0, 128)
        ],
        axis=0,
    )


def from_points(points):
    half = 2 * HEIGHT
    return jnp.concatenate(
        [
            jnp.concatenate([points[at : at + half, :128], points[at : at + half, 128:]], axis=0)
            for at in (0, half)
        ],
        axis=1,
    )


def is_packed(q):
    return jnp.where(lax.axis_index("lat") == 0, 1, 0) if q == 0 else 0


def filter_kernel(
    wire, forward, inverse, weight1, bias1, weight2, bias2,
    wire_back, slopes_out, squares_out,
    slopes, squares, scratch, columns, backs, square, w1, w2, c1, c2, sem,
):
    build_weight(weight1, square, w1)
    build_weight(weight2, square, w2)
    build_bias(bias1, c1)
    build_bias(bias2, c2)
    spectrum_in(wire, scratch, columns)

    for q in range(ROWS):
        which = is_packed(q)
        points = to_points(dot(forward[which], columns[q]).astype(BF16))
        active, slope = gelu_pair(dot(points, w1[...]) + c1[...])
        slopes[q] = slope.astype(BF16)
        post = dot(active.astype(BF16), w2[...]) + c2[...]
        bend = jnp.tanh(post * (1.0 / THRESHOLD))
        squares[q] = (bend * bend).astype(BF16)
        shrunk = from_points((post - THRESHOLD * bend).astype(BF16))
        backs[q] = dot(inverse[which], shrunk)

    keep = fetch(sem, (slopes, slopes_out), (squares, squares_out))
    spectrum_out(backs, scratch, wire_back)
    keep(0, 1)


def adjoint_kernel(
    wire, forward, inverse, weight1, weight2, slopes, squares,
    wire_back,
    scratch, columns, backs, square, w1, w2,
):
    build_weight(weight1, square, w1)
    build_weight(weight2, square, w2)
    spectrum_in(wire, scratch, columns)

    for q in range(ROWS):
        which = is_packed(q)
        spectrum = dot(forward[which], columns[q])
        points = (to_points(spectrum) * squares[q].astype(F32)).astype(BF16)
        pre = (dot_t(points, w2[...]) * slopes[q].astype(F32)).astype(BF16)
        shrunk = from_points(dot_t(pre, w1[...]).astype(BF16))
        backs[q] = dot(inverse[which], shrunk)

    spectrum_out(backs, scratch, wire_back)


def pieces(n):
    return pl.ds(CHUNK * n if isinstance(n, int) else pl.multiple_of(CHUNK * n, CHUNK), CHUNK)


def chunk_copies(sem, copy):
    one = lambda n: pltpu.make_async_copy(*copy(pieces(n)), sem.at[n])
    return lambda n: one(n).start(), lambda n: one(n).wait()


def gradient_kernel(
    cotangents, states, gain1s, shift1s, gain2s, shift2s, bias1s, fc2s,
    grad_hiddens, base, cotangent, gain2, shift2, bias1,
    state, gain1, shift1, fc2, grad_hidden, sem, sem_in, sem_out,
):
    wait = fetch(
        sem, (cotangents, cotangent), (states, state), (gain1s, gain1), (shift1s, shift1),
        (gain2s, gain2), (shift2s, shift2), (bias1s, bias1),
    )
    start_in, wait_in = chunk_copies(sem_in, lambda c: (fc2s.at[c, :], fc2.at[c, :]))
    start_out, wait_out = chunk_copies(sem_out, lambda c: (grad_hidden.at[:, c], grad_hiddens.at[:, c]))
    pl.loop(0, CHUNKS)(start_in)
    wait(*range(7))
    for batch in range(BATCHES):
        rows = batch_rows(batch)
        value = state[rows, :].astype(F32)
        normed, _ = norm(value)
        base[rows, :] = (normed * row(gain1) + row(shift1)).astype(BF16).astype(F32) + value

    @pl.loop(0, CHUNKS)
    def _(n):
        wait_in(n)
        grad_hidden[:, pieces(n)] = dot_t(cotangent[...], fc2[pieces(n), :]).astype(BF16)
        start_out(n)

    pl.loop(0, CHUNKS)(wait_out)


def token_kernel(
    wire, base, cotangent, gain, shift, bias1, fc1s, grad_hiddens,
    hiddens, mixeds, grad_mixed, wire_next,
    fc1, grad_hidden, hidden, mixed, blocks, rows_in, grad_total, sem, sem_fc1, sem_grad, sem_hidden,
):
    start_fc1, wait_fc1 = chunk_copies(sem_fc1, lambda c: (fc1s.at[:, c], fc1.at[:, c]))
    start_grad, wait_grad = chunk_copies(sem_grad, lambda c: (grad_hiddens.at[:, c], grad_hidden.at[:, c]))
    start_hidden, wait_hidden = chunk_copies(sem_hidden, lambda c: (hidden.at[:, c], hiddens.at[:, c]))

    @pl.loop(0, CHUNKS)
    def _(n):
        start_fc1(n)
        start_grad(n)

    receive_blocks(wire, blocks)
    for batch in range(BATCHES):
        rows = batch_rows(batch)
        value = (gather_blocks(blocks, batch) + base[rows, :]).astype(BF16)
        mixed[rows, :] = value
        normed, _ = norm(value.astype(F32))
        rows_in[rows, :] = (normed * row(gain) + row(shift)).astype(BF16)
    keep = fetch(sem, (mixed, mixeds))
    grad_total[...] = jnp.zeros_like(grad_total)

    @pl.loop(0, CHUNKS)
    def _(n):
        wait_fc1(n)
        hidden_pre = dot(rows_in[...], fc1[:, pieces(n)]) + bias1[:, pieces(n)]
        value, slope = gelu_pair(hidden_pre)
        hidden[:, pieces(n)] = value.astype(BF16)
        start_hidden(n)
        wait_grad(n)
        grad_pre = (grad_hidden[:, pieces(n)].astype(F32) * slope).astype(BF16)
        grad_total[...] += dot_t(grad_pre, fc1[:, pieces(n)])

    for batch in range(BATCHES):
        rows = batch_rows(batch)
        normed, scale = norm(mixed[rows, :].astype(F32))
        grad = cotangent[rows, :].astype(F32) + norm_backward(grad_total[rows, :], row(gain), normed, scale)
        grad = grad.astype(BF16)
        grad_mixed[rows, :] = grad
        scatter_blocks(blocks, batch, grad.astype(F32))
    send_blocks(blocks, wire_next)
    keep(0)
    pl.loop(0, CHUNKS)(wait_hidden)


def advance_kernel(
    hiddens, fc2s, bias2s, mixeds, states,
    advanced, normed, scale,
    hidden, fc2, bias2, mixed, state, total, sem, sem_hidden, sem_fc2,
):
    wait = fetch(sem, (bias2s, bias2), (mixeds, mixed), (states, state))
    start_hidden, wait_hidden = chunk_copies(sem_hidden, lambda c: (hiddens.at[:, c], hidden.at[:, c]))
    start_fc2, wait_fc2 = chunk_copies(sem_fc2, lambda c: (fc2s.at[c, :], fc2.at[c, :]))

    @pl.loop(0, CHUNKS)
    def _(n):
        start_hidden(n)
        start_fc2(n)

    wait(0, 1, 2)
    for batch in range(BATCHES):
        rows = batch_rows(batch)
        normed[rows, :], scale[rows, :] = norm(state[rows, :].astype(F32))
    total[...] = mixed[...].astype(F32) + row(bias2)

    @pl.loop(0, CHUNKS)
    def _(n):
        wait_hidden(n)
        wait_fc2(n)
        total[...] += dot(hidden[:, pieces(n)], fc2[pieces(n), :])

    advanced[...] = total[...].astype(BF16)


def finish_kernel(wire, normed, scale, grad_mixed, gain, sensitivity, blocks, out, sem_out):
    receive_blocks(wire, blocks)
    copies = []
    for batch in range(BATCHES):
        rows = batch_rows(batch)
        grad = grad_mixed[rows, :].astype(F32)
        grad_lowered = gather_blocks(blocks, batch) + grad
        grad = grad + norm_backward(grad_lowered, row(gain), normed[rows, :], scale[rows, :])
        out[rows, :] = grad.astype(BF16)
        copies.append(pltpu.make_async_copy(out.at[rows, :], sensitivity.at[rows, :], sem_out.at[batch]))
        copies[-1].start()
    for c in copies:
        c.wait()


def near(*shape, dtype=BF16):
    return jax.ShapeDtypeStruct(shape, dtype)


def vmem(*shape, dtype=BF16):
    return pltpu.VMEM(shape, dtype)


def sems(n):
    return pltpu.SemaphoreType.DMA((n,))


LON_WIRE = near(LONS, COLS, LANES)
FIELD = near(WIDTH, LANES)
LAT_WIRE = near(LATS, WIRE, 128)
BLOCKS = vmem(LONS, GROUPS, COLS, 128, dtype=F32)
PEERS = vmem(LATS * STRIDE, 128, dtype=F32)
POINTS = (ROWS, 4 * HEIGHT, 256)
SPECTRAL = (
    PEERS,
    vmem(ROWS, 2 * HEIGHT, 256),
    vmem(ROWS, 2 * HEIGHT, 256, dtype=F32),
    vmem(256, 256, dtype=F32),
    vmem(256, 256),
    vmem(256, 256),
)
WIDE_BIAS = vmem(1, 256, dtype=F32)
TOKEN, UNITS = (TOKENS, FEATURES), (TOKENS, HIDDEN)
VECTOR = vmem(FEATURES, dtype=F32)
PARAMS = pltpu.CompilerParams(vmem_limit_bytes=48 * 1024 * 1024)
MATMUL = 2 * TOKENS * FEATURES * HIDDEN


def place(space):
    return pl.BlockSpec() if space is None else pl.BlockSpec(memory_space=space)


def call(kernel, out_shape, scratch, operands, places, flops=0):
    single = not isinstance(out_shape, tuple)
    shapes = (out_shape,) if single else out_shape
    specs = tuple(place(None if isinstance(o, jax.ShapeDtypeStruct) else o.memory_space) for o in shapes)
    spaces = [{"f": pltpu.HBM, "h": pltpu.VMEM, "n": None}[p] for p in places]
    return pl.pallas_call(
        kernel,
        out_shape=out_shape,
        in_specs=[place(m) for m in spaces],
        out_specs=specs[0] if single else specs,
        scratch_shapes=scratch,
        name=kernel.__name__,
        compiler_params=PARAMS,
        cost_estimate=pl.CostEstimate(flops=flops, bytes_accessed=0, transcendentals=0),
    )(*(v if m is None else pltpu.with_memory_space_constraint(v, m) for v, m in zip(operands, spaces, strict=True)))


def exchange(value, axis):
    return lax.all_to_all(value, axis, split_axis=0, concat_axis=0, tiled=True)


def to_lat(wire, table):
    field = exchange(wire, "lon").reshape(WIDTH, LANES)
    return exchange(call(width_kernel, LAT_WIRE, [PEERS], [field, table], "nh"), "lat")


def to_lon(wire, table):
    scratch = [PEERS, vmem(WIDTH, LANES)]
    field = call(width_back_kernel, FIELD, scratch, [exchange(wire, "lat"), table], "nh")
    return exchange(field.reshape(LON_WIRE.shape), "lon")


def begin(*operands):
    return call(
        begin_kernel,
        LON_WIRE,
        [vmem(*TOKEN), VECTOR, VECTOR, BLOCKS, sems(3)],
        operands,
        "fff",
    )


def keep(*arrays):
    shapes = tuple(vmem(*k.shape, dtype=k.dtype) for k in arrays)
    return call(keep_kernel, shapes, [sems(len(arrays))], arrays, "f" * len(arrays), MATMUL)


def filtered(wire, *kept):
    return call(
        filter_kernel,
        (LAT_WIRE, pltpu.HBM(POINTS, BF16), pltpu.HBM(POINTS, BF16)),
        [vmem(*POINTS), vmem(*POINTS), *SPECTRAL, WIDE_BIAS, WIDE_BIAS, sems(2)],
        [wire, *kept],
        "nhhhhhh",
    )


def adjoint(wire, *operands):
    return call(adjoint_kernel, LAT_WIRE, [*SPECTRAL], [wire, *operands], "nhhhhnn")


def gradient(*operands):
    return call(
        gradient_kernel,
        (pltpu.HBM(UNITS, BF16), vmem(*TOKEN, dtype=F32), vmem(*TOKEN), VECTOR, VECTOR, vmem(1, HIDDEN, dtype=F32)),
        [vmem(*TOKEN), VECTOR, VECTOR, vmem(HIDDEN, FEATURES), vmem(*UNITS)]
        + [sems(7), sems(CHUNKS), sems(CHUNKS)],
        operands,
        "ffffffff",
        MATMUL,
    )


def token(*operands):
    return call(
        token_kernel,
        (pltpu.HBM(UNITS, BF16), pltpu.HBM(TOKEN, BF16), vmem(*TOKEN), LON_WIRE),
        [vmem(FEATURES, HIDDEN), vmem(*UNITS), vmem(*UNITS), vmem(*TOKEN), BLOCKS, vmem(*TOKEN)]
        + [vmem(*TOKEN, dtype=F32), sems(1), sems(CHUNKS), sems(CHUNKS), sems(CHUNKS)],
        operands,
        "nhhhhhff",
        2 * MATMUL,
    )


def advance(*operands):
    return call(
        advance_kernel,
        (near(*TOKEN), vmem(*TOKEN, dtype=F32), vmem(TOKENS, 1, dtype=F32)),
        [vmem(*UNITS), vmem(HIDDEN, FEATURES), VECTOR, vmem(*TOKEN), vmem(*TOKEN), vmem(*TOKEN, dtype=F32)]
        + [sems(3), sems(CHUNKS), sems(CHUNKS)],
        operands,
        "fffff",
        MATMUL,
    )


def finish(*operands):
    return call(
        finish_kernel,
        pltpu.HBM(TOKEN, BF16),
        [BLOCKS, vmem(*TOKEN), sems(BATCHES)],
        operands,
        "nhhhh",
    )


def shards(
    state, spec_weight1, spec_bias1, spec_weight2, spec_bias2, norm1_gain, norm1_bias, norm2_gain, norm2_bias,
    fc1_weight, fc1_bias, fc2_weight, fc2_bias, cotangent,
):
    tokens = state.reshape(TOKEN)
    cot = cotangent.reshape(TOKEN)
    tables = map(jnp.asarray, (*width_tables(), *height_tables()))
    weight1, weight2 = spec_weight1.reshape(2, BLOCK, BLOCK), spec_weight2.reshape(2, BLOCK, BLOCK)
    bias1, bias2 = spec_bias1.reshape(2, BLOCK), spec_bias2.reshape(2, BLOCK)

    wire = begin(tokens, norm1_gain, norm1_bias)
    width_forward, width_inverse, height_forward, height_inverse, weight1, weight2, bias1, bias2, gain1 = keep(
        *tables, weight1, weight2, bias1, bias2, norm1_gain
    )
    wire = to_lat(wire, width_forward)
    wire, slopes, squares = filtered(wire, height_forward, height_inverse, weight1, bias1, weight2, bias2)
    grad_hidden, base, cot, gain2, shift2, fc1_bias = gradient(
        cot, tokens, norm1_gain, norm1_bias, norm2_gain, norm2_bias, fc1_bias.reshape(1, -1), fc2_weight
    )
    wire = to_lon(wire, width_inverse)
    hidden, mixed, grad_mixed, wire = token(wire, base, cot, gain2, shift2, fc1_bias, fc1_weight, grad_hidden)
    wire = to_lat(wire, width_forward)
    wire = adjoint(wire, height_forward, height_inverse, weight1, weight2, slopes, squares)
    advanced, normed, scale = advance(hidden, fc2_weight, fc2_bias, mixed, tokens)
    wire = to_lon(wire, width_inverse)
    sensitivity = finish(wire, normed, scale, grad_mixed, gain1)
    return advanced.reshape(state.shape), sensitivity.reshape(state.shape)


def solution(mesh):
    field = P("ens", "lat", "lon", None)
    block, bias = P(None, "lon", None, None), P(None, "lon", None)
    return jax.shard_map(
        shards,
        mesh=mesh,
        in_specs=(field, block, bias, block, bias, *[P()] * 8, field),
        out_specs=(field, field),
        check_vma=False,
    )
```

```python
import math

import jax
import jax.numpy as jnp
import numpy as np
from jax import lax
from jax.experimental import pallas as pl
from jax.experimental.pallas import tpu as pltpu
from jax.sharding import PartitionSpec as P

EPSILON = 1e-06
THRESHOLD = 0.01
LATS, LONS = 16, 8
HEIGHT, WIDTH, FEATURES, HIDDEN = 96, 192, 768, 3072
ROWS, COLS = HEIGHT // LATS, WIDTH // LONS
BLOCK = FEATURES // LONS
STATES = 2
GROUPS = STATES * ROWS
TOKENS = GROUPS * COLS
LANES = GROUPS * BLOCK
TILES = LANES // 128
WIRE = TILES * GROUPS
STRIDE = 109
CHUNK = 1024
STEP = 256
BATCH = 6
BATCHES = GROUPS // BATCH
CHUNKS = HIDDEN // CHUNK
F32, BF16 = jnp.float32, jnp.bfloat16


def split_table(table):
    high = table.astype(BF16)
    return np.stack([high, (table - high.astype(np.float64)).astype(BF16)])


def width_tables():
    part, q, d = np.meshgrid(np.arange(2), np.arange(ROWS), np.arange(LATS), indexing="ij")
    part, freq = part.reshape(-1, 1), (q + ROWS * d).reshape(-1, 1)
    w = np.arange(WIDTH).reshape(1, -1)
    angle = 2.0 * math.pi * (freq * w % WIDTH) / WIDTH
    parity = np.where(w % 2 == 0, 1.0, -1.0)
    scale = 1.0 / math.sqrt(WIDTH)
    forward = np.where(part == 0, np.cos(angle), np.where(freq == 0, parity, -np.sin(angle)))
    twice = np.where(freq == 0, 1.0, 2.0)
    return split_table(forward * scale), split_table((forward * twice * scale).T)


def height_tables():
    p = np.arange(HEIGHT).reshape(-1, 1, 1)
    r = np.arange(ROWS).reshape(1, -1, 1)
    s = np.arange(LATS).reshape(1, 1, -1)
    angle = 2.0 * math.pi * (p * (ROWS * s + r) % HEIGHT) / HEIGHT
    c, n = np.cos(angle) / math.sqrt(HEIGHT), np.sin(angle) / math.sqrt(HEIGHT)
    zero = np.zeros_like(c)

    def join(rows):
        return np.concatenate([np.stack(row, axis=2).reshape(HEIGHT, -1) for row in rows], axis=0)

    plain = join([[c, n], [c, n], [-n, c], [n, -c]])
    packed = join([[c, zero], [zero, c], [-n, zero], [zero, -n]])

    def join_back(rows):
        return np.concatenate(
            [np.concatenate([v.reshape(HEIGHT, -1).T for v in row], axis=1) for row in rows], axis=0
        )

    h = 0.5
    plain_back = join_back([[h * c, h * c, -h * n, h * n], [h * n, h * n, h * c, -h * c]])
    packed_back = join_back([[c, zero, -n, zero], [zero, c, zero, -n]])
    return np.stack([plain, packed]).astype(BF16), np.stack([plain_back, packed_back]).astype(BF16)


def dot(a, b):
    return lax.dot_general(a, b, (((1,), (0,)), ((), ())), preferred_element_type=F32)


def dot_t(a, b):
    return lax.dot_general(a, b, (((1,), (1,)), ((), ())), preferred_element_type=F32)


def lane_index(rows):
    return lax.broadcasted_iota(jnp.int32, (rows, 128), 1)


def unpack4(t0, t1, t2):
    lane = lane_index(t0.shape[0])
    b1 = jnp.where(lane < 32, pltpu.roll(t0, 32, 1), pltpu.roll(t1, 32, 1))
    b2 = jnp.where(lane < 64, pltpu.roll(t1, 64, 1), pltpu.roll(t2, 64, 1))
    return t0, b1, b2, pltpu.roll(t2, 96, 1)


def pack4(b0, b1, b2, b3):
    lane = lane_index(b0.shape[0])
    r1, r2, r3 = pltpu.roll(b1, 96, 1), pltpu.roll(b2, 64, 1), pltpu.roll(b3, 32, 1)
    return (
        jnp.where(lane < 96, b0, r1),
        jnp.where(lane < 64, r1, r2),
        jnp.where(lane < 32, r2, r3),
    )


def row(vector):
    return vector[...].reshape(1, -1)


def norm(values):
    average = jnp.mean(values, axis=-1, keepdims=True)
    centred = values - average
    inverse = lax.rsqrt(jnp.mean(centred * centred, axis=-1, keepdims=True) + EPSILON)
    return centred * inverse, inverse


def norm_backward(gradient, gain, normed, inverse):
    scaled = gradient * gain
    return inverse * (
        scaled
        - jnp.mean(scaled, axis=-1, keepdims=True)
        - normed * jnp.mean(scaled * normed, axis=-1, keepdims=True)
    )


def gelu_pair(values):
    cumulative = 0.5 * (1.0 + lax.erf(values * 0.7071067811865476))
    density = jnp.exp(-0.5 * values * values) * 0.3989422804014327
    return values * cumulative, cumulative + values * density


def scatter_blocks(blocks, batch, values):
    tiles = [values[:, 128 * i : 128 * i + 128] for i in range(6)]
    for j, b in enumerate((*unpack4(*tiles[:3]), *unpack4(*tiles[3:]))):
        for n in range(BATCH):
            blocks[j, BATCH * batch + n] = b[COLS * n : COLS * n + COLS]


def send_blocks(blocks, wire):
    for j in range(LONS):
        for g in range(GROUPS // 4):
            tiles = pack4(*(blocks[j, 4 * g + n] for n in range(4)))
            for i, t in enumerate(tiles):
                at = 384 * g + 128 * i
                wire[j, :, at : at + 128] = t.astype(BF16)


def receive_blocks(wire, blocks):
    for j in range(LONS):
        for g in range(GROUPS // 4):
            at = 384 * g
            tiles = [wire[j, :, at + 128 * i : at + 128 * i + 128].astype(F32) for i in range(3)]
            for n, b in enumerate(unpack4(*tiles)):
                blocks[j, 4 * g + n] = b


def gather_blocks(blocks, batch):
    groups = range(BATCH * batch, BATCH * batch + BATCH)
    parts = [jnp.concatenate([blocks[j, k] for k in groups], axis=0) for j in range(LONS)]
    return jnp.concatenate([*pack4(*parts[:4]), *pack4(*parts[4:])], axis=1)


def fetch(sem, *pairs):
    copies = [pltpu.make_async_copy(source, target, sem.at[n]) for n, (source, target) in enumerate(pairs)]
    for c in copies:
        c.start()

    def wait(*numbers):
        for n in numbers:
            copies[n].wait()

    return wait


def batch_rows(batch):
    size = BATCH * COLS
    return slice(size * batch, size * batch + size)


def begin_kernel(states, gains, shifts, wire, state, gain, shift, blocks, sem):
    fetch(sem, (states, state), (gains, gain), (shifts, shift))(0, 1, 2)
    for batch in range(BATCHES):
        normed, _ = norm(state[batch_rows(batch), :].astype(F32))
        value = (normed * row(gain) + row(shift)).astype(BF16)
        scatter_blocks(blocks, batch, value.astype(F32))
    send_blocks(blocks, wire)


def wire_out(scratch, wire):
    for d in range(LATS):
        wire[d] = scratch[STRIDE * d : STRIDE * d + WIRE, :].astype(BF16)


def wire_in(wire, scratch):
    for d in range(LATS):
        scratch[STRIDE * d : STRIDE * d + WIRE, :] = wire[d].astype(F32)


def peers(row):
    return pl.ds(row, LATS, stride=STRIDE)


def width_kernel(field, table, wire, scratch):
    product = dot(table[0], field[...]) + dot(table[1], field[...])
    for e in range(GROUPS):
        for i in range(TILES):
            scratch[peers(GROUPS * i + e), :] = product[16 * e : 16 * e + 16, 128 * i : 128 * i + 128]
    wire_out(scratch, wire)


def width_back_kernel(wire, table, field, scratch, gathered):
    wire_in(wire, scratch)
    for e in range(GROUPS):
        for i in range(TILES):
            piece = scratch[peers(GROUPS * i + e), :]
            gathered[16 * e : 16 * e + 16, 128 * i : 128 * i + 128] = piece.astype(BF16)
    field[...] = (dot(table[0], gathered[...]) + dot(table[1], gathered[...])).astype(BF16)


def spectrum_in(wire, scratch, columns):
    wire_in(wire, scratch)
    for part in range(2):
        for q in range(ROWS):
            e = ROWS * part + q
            for g in range(GROUPS // 4):
                tiles = [scratch[peers(GROUPS * (3 * g + i) + e), :] for i in range(3)]
                for n, b in enumerate(unpack4(*tiles)):
                    state, r = divmod(4 * g + n, ROWS)
                    at = 16 * (2 * r + part)
                    columns[q, at : at + 16, 128 * state : 128 * state + 128] = b.astype(BF16)


def spectrum_out(backs, scratch, wire):
    for part in range(2):
        for q in range(ROWS):
            e = ROWS * part + q
            for g in range(GROUPS // 4):
                blocks = []
                for n in range(4):
                    state, r = divmod(4 * g + n, ROWS)
                    at = 16 * (ROWS * part + r)
                    blocks.append(backs[q, at : at + 16, 128 * state : 128 * state + 128])
                for i, t in enumerate(pack4(*blocks)):
                    scratch[peers(GROUPS * (3 * g + i) + e), :] = t
    wire_out(scratch, wire)


def build_weight(weight, square, out):
    square[...] = jnp.zeros_like(square)
    square[0:BLOCK, 0:BLOCK] = weight[0]
    square[0:BLOCK, 128 : 128 + BLOCK] = weight[1]
    square[128 : 128 + BLOCK, 0:BLOCK] = -weight[1]
    square[128 : 128 + BLOCK, 128 : 128 + BLOCK] = weight[0]
    out[...] = square[...].astype(BF16)


def build_bias(bias, out):
    out[...] = jnp.zeros_like(out)
    out[0:1, 0:BLOCK] = bias[0:1, :]
    out[0:1, 128 : 128 + BLOCK] = bias[1:2, :]


def to_points(spectrum):
    half = 2 * HEIGHT
    return jnp.concatenate(
        [
            jnp.concatenate([spectrum[:half, at : at + 128], spectrum[half:, at : at + 128]], axis=1)
            for at in (0, 128)
        ],
        axis=0,
    )


def from_points(points):
    half = 2 * HEIGHT
    return jnp.concatenate(
        [
            jnp.concatenate([points[at : at + half, :128], points[at : at + half, 128:]], axis=0)
            for at in (0, half)
        ],
        axis=1,
    )


def is_packed(q):
    return jnp.where(lax.axis_index("lat") == 0, 1, 0) if q == 0 else 0


def filter_kernel(
    wire, forward, inverse, weight1, bias1, weight2, bias2,
    wire_back, slopes_out, squares_out,
    slopes, squares, scratch, columns, backs, square, w1, w2, c1, c2, sem,
):
    build_weight(weight1, square, w1)
    build_weight(weight2, square, w2)
    build_bias(bias1, c1)
    build_bias(bias2, c2)
    spectrum_in(wire, scratch, columns)

    for q in range(ROWS):
        which = is_packed(q)
        points = to_points(dot(forward[which], columns[q]).astype(BF16))
        active, slope = gelu_pair(dot(points, w1[...]) + c1[...])
        slopes[q] = slope.astype(BF16)
        post = dot(active.astype(BF16), w2[...]) + c2[...]
        bend = jnp.tanh(post * (1.0 / THRESHOLD))
        squares[q] = (bend * bend).astype(BF16)
        shrunk = from_points((post - THRESHOLD * bend).astype(BF16))
        backs[q] = dot(inverse[which], shrunk)

    keep = fetch(sem, (slopes, slopes_out), (squares, squares_out))
    spectrum_out(backs, scratch, wire_back)
    keep(0, 1)


def adjoint_kernel(
    wire, forward, inverse, weight1, weight2, slopes, squares,
    wire_back,
    scratch, columns, backs, square, w1, w2,
):
    build_weight(weight1, square, w1)
    build_weight(weight2, square, w2)
    spectrum_in(wire, scratch, columns)

    for q in range(ROWS):
        which = is_packed(q)
        spectrum = dot(forward[which], columns[q])
        points = (to_points(spectrum) * squares[q].astype(F32)).astype(BF16)
        pre = (dot_t(points, w2[...]) * slopes[q].astype(F32)).astype(BF16)
        shrunk = from_points(dot_t(pre, w1[...]).astype(BF16))
        backs[q] = dot(inverse[which], shrunk)

    spectrum_out(backs, scratch, wire_back)


def pieces(n):
    return pl.ds(CHUNK * n if isinstance(n, int) else pl.multiple_of(CHUNK * n, CHUNK), CHUNK)


def chunk_copies(sem, copy):
    one = lambda n: pltpu.make_async_copy(*copy(pieces(n)), sem.at[n])
    return lambda n: one(n).start(), lambda n: one(n).wait()


def gradient_kernel(cotangents, states, shift1s, fc2s, gain1s, *refs):
    more, (grad_hiddens, base, cotangent), rest = refs[:HELD], refs[HELD : HELD + 3], refs[HELD + 3 :]
    gain1, held, (state, shift1, fc2, grad_hidden, sem, sem_in, sem_out) = rest[0], rest[1 : HELD + 1], rest[HELD + 1 :]
    wait = fetch(
        sem, (cotangents, cotangent), (states, state), (gain1s, gain1), (shift1s, shift1),
        *zip(more, held, strict=True),
    )
    start_in, wait_in = chunk_copies(sem_in, lambda c: (fc2s.at[c, :], fc2.at[c, :]))
    start_out, wait_out = chunk_copies(sem_out, lambda c: (grad_hidden.at[:, c], grad_hiddens.at[:, c]))
    pl.loop(0, CHUNKS)(start_in)
    wait(*range(4 + HELD))
    for batch in range(BATCHES):
        rows = batch_rows(batch)
        value = state[rows, :].astype(F32)
        normed, _ = norm(value)
        base[rows, :] = (normed * row(gain1) + row(shift1)).astype(BF16).astype(F32) + value

    @pl.loop(0, CHUNKS)
    def _(n):
        wait_in(n)
        grad_hidden[:, pieces(n)] = dot_t(cotangent[...], fc2[pieces(n), :]).astype(BF16)
        start_out(n)

    pl.loop(0, CHUNKS)(wait_out)


def token_kernel(
    wire, base, cotangent, gain, shift, bias1, fc1s, grad_hidden,
    hiddens, mixeds, grad_mixed, wire_next,
    fc1, hidden, mixed, blocks, rows_in, grad_pre, grad_total, sem, sem_fc1, sem_hidden,
):
    start_fc1, wait_fc1 = chunk_copies(sem_fc1, lambda c: (fc1s.at[:, c], fc1.at[:, c]))
    start_hidden, wait_hidden = chunk_copies(sem_hidden, lambda c: (hidden.at[:, c], hiddens.at[:, c]))

    pl.loop(0, CHUNKS)(start_fc1)
    receive_blocks(wire, blocks)
    for batch in range(BATCHES):
        rows = batch_rows(batch)
        value = (gather_blocks(blocks, batch) + base[rows, :]).astype(BF16)
        mixed[rows, :] = value
        normed, _ = norm(value.astype(F32))
        rows_in[rows, :] = (normed * row(gain) + row(shift)).astype(BF16)
    keep = fetch(sem, (mixed, mixeds))

    def units(n):
        return slice(STEP * n, STEP * n + STEP)

    def before(n):
        if STEP * n % CHUNK == 0:
            wait_fc1(STEP * n // CHUNK)
        return dot(rows_in[...], fc1[:, units(n)]) + bias1[:, units(n)]

    hidden_pre = before(0)
    for n in range(HIDDEN // STEP):
        following = before(n + 1) if n + 1 < HIDDEN // STEP else None
        value, slope = gelu_pair(hidden_pre)
        hidden[:, units(n)] = value.astype(BF16)
        grad_pre[:, units(n)] = (grad_hidden[:, units(n)].astype(F32) * slope).astype(BF16)
        if (STEP * n + STEP) % CHUNK == 0:
            start_hidden(STEP * n // CHUNK)
        hidden_pre = following
    grad_total[...] = dot_t(grad_pre[...], fc1[...])

    for batch in range(BATCHES):
        rows = batch_rows(batch)
        normed, scale = norm(mixed[rows, :].astype(F32))
        grad = cotangent[rows, :].astype(F32) + norm_backward(grad_total[rows, :], row(gain), normed, scale)
        grad = grad.astype(BF16)
        grad_mixed[rows, :] = grad
        scatter_blocks(blocks, batch, grad.astype(F32))
    send_blocks(blocks, wire_next)
    keep(0)
    pl.loop(0, CHUNKS)(wait_hidden)


def advance_kernel(
    hiddens, fc2s, bias2s, mixeds, states,
    advanced, normed, scale,
    hidden, fc2, bias2, mixed, state, total, sem, sem_hidden, sem_fc2,
):
    wait = fetch(sem, (bias2s, bias2), (mixeds, mixed), (states, state))
    start_hidden, wait_hidden = chunk_copies(sem_hidden, lambda c: (hiddens.at[:, c], hidden.at[:, c]))
    start_fc2, wait_fc2 = chunk_copies(sem_fc2, lambda c: (fc2s.at[c, :], fc2.at[c, :]))

    @pl.loop(0, CHUNKS)
    def _(n):
        start_hidden(n)
        start_fc2(n)

    wait(0, 1, 2)
    for batch in range(BATCHES):
        rows = batch_rows(batch)
        normed[rows, :], scale[rows, :] = norm(state[rows, :].astype(F32))
    total[...] = mixed[...].astype(F32) + row(bias2)

    @pl.loop(0, CHUNKS)
    def _(n):
        wait_hidden(n)
        wait_fc2(n)
        total[...] += dot(hidden[:, pieces(n)], fc2[pieces(n), :])

    advanced[...] = total[...].astype(BF16)


def finish_kernel(wire, normed, scale, grad_mixed, gain, sensitivity, blocks, out, sem_out):
    receive_blocks(wire, blocks)
    copies = []
    for batch in range(BATCHES):
        rows = batch_rows(batch)
        grad = grad_mixed[rows, :].astype(F32)
        grad_lowered = gather_blocks(blocks, batch) + grad
        grad = grad + norm_backward(grad_lowered, row(gain), normed[rows, :], scale[rows, :])
        out[rows, :] = grad.astype(BF16)
        copies.append(pltpu.make_async_copy(out.at[rows, :], sensitivity.at[rows, :], sem_out.at[batch]))
        copies[-1].start()
    for c in copies:
        c.wait()


def near(*shape, dtype=BF16):
    return jax.ShapeDtypeStruct(shape, dtype)


def vmem(*shape, dtype=BF16):
    return pltpu.VMEM(shape, dtype)


def sems(n):
    return pltpu.SemaphoreType.DMA((n,))


LON_WIRE = near(LONS, COLS, LANES)
FIELD = near(WIDTH, LANES)
LAT_WIRE = near(LATS, WIRE, 128)
BLOCKS = vmem(LONS, GROUPS, COLS, 128, dtype=F32)
PEERS = vmem(LATS * STRIDE, 128, dtype=F32)
POINTS = (ROWS, 4 * HEIGHT, 256)
SPECTRAL = (
    PEERS,
    vmem(ROWS, 2 * HEIGHT, 256),
    vmem(ROWS, 2 * HEIGHT, 256, dtype=F32),
    vmem(256, 256, dtype=F32),
    vmem(256, 256),
    vmem(256, 256),
)
WIDE_BIAS = vmem(1, 256, dtype=F32)
TOKEN, UNITS = (TOKENS, FEATURES), (TOKENS, HIDDEN)
VECTOR = vmem(FEATURES, dtype=F32)
PARAMS = pltpu.CompilerParams(vmem_limit_bytes=48 * 1024 * 1024)
HELD = 11
MATMUL = 2 * TOKENS * FEATURES * HIDDEN


def place(space):
    return pl.BlockSpec() if space is None else pl.BlockSpec(memory_space=space)


def call(kernel, out_shape, scratch, operands, places, flops=0):
    single = not isinstance(out_shape, tuple)
    shapes = (out_shape,) if single else out_shape
    specs = tuple(place(None if isinstance(o, jax.ShapeDtypeStruct) else o.memory_space) for o in shapes)
    spaces = [{"f": pltpu.HBM, "h": pltpu.VMEM, "n": None}[p] for p in places]
    return pl.pallas_call(
        kernel,
        out_shape=out_shape,
        in_specs=[place(m) for m in spaces],
        out_specs=specs[0] if single else specs,
        scratch_shapes=scratch,
        name=kernel.__name__,
        compiler_params=PARAMS,
        cost_estimate=pl.CostEstimate(flops=flops, bytes_accessed=0, transcendentals=0),
    )(*(v if m is None else pltpu.with_memory_space_constraint(v, m) for v, m in zip(operands, spaces, strict=True)))


def exchange(value, axis):
    return lax.all_to_all(value, axis, split_axis=0, concat_axis=0, tiled=True)


def to_lat(wire, table):
    field = exchange(wire, "lon").reshape(WIDTH, LANES)
    return exchange(call(width_kernel, LAT_WIRE, [PEERS], [field, table], "nh"), "lat")


def to_lon(wire, table):
    scratch = [PEERS, vmem(WIDTH, LANES)]
    field = call(width_back_kernel, FIELD, scratch, [exchange(wire, "lat"), table], "nh")
    return exchange(field.reshape(LON_WIRE.shape), "lon")


def begin(*operands):
    return call(
        begin_kernel,
        LON_WIRE,
        [vmem(*TOKEN), VECTOR, VECTOR, BLOCKS, sems(3)],
        operands,
        "fff",
    )


def filtered(wire, *kept):
    return call(
        filter_kernel,
        (LAT_WIRE, pltpu.HBM(POINTS, BF16), pltpu.HBM(POINTS, BF16)),
        [vmem(*POINTS), vmem(*POINTS), *SPECTRAL, WIDE_BIAS, WIDE_BIAS, sems(2)],
        [wire, *kept],
        "nhhhhhh",
    )


def adjoint(wire, *operands):
    return call(adjoint_kernel, LAT_WIRE, [*SPECTRAL], [wire, *operands], "nhhhhnn")


def gradient(cot, tokens, shift1, fc2, gain1, *arrays):
    return call(
        gradient_kernel,
        (pltpu.HBM(UNITS, BF16), vmem(*TOKEN, dtype=F32), vmem(*TOKEN))
        + tuple(vmem(*a.shape, dtype=a.dtype) for a in (gain1, *arrays)),
        [vmem(*TOKEN), VECTOR, vmem(HIDDEN, FEATURES), vmem(*UNITS), sems(4 + HELD), sems(CHUNKS), sems(CHUNKS)],
        [cot, tokens, shift1, fc2, gain1, *arrays],
        "fffff" + "f" * len(arrays),
        MATMUL,
    )


def token(*operands):
    return call(
        token_kernel,
        (pltpu.HBM(UNITS, BF16), pltpu.HBM(TOKEN, BF16), vmem(*TOKEN), LON_WIRE),
        [vmem(FEATURES, HIDDEN), vmem(*UNITS), vmem(*TOKEN), BLOCKS, vmem(*TOKEN)]
        + [vmem(*UNITS), vmem(*TOKEN, dtype=F32), sems(1), sems(CHUNKS), sems(CHUNKS)],
        operands,
        "nhhhhhfh",
        2 * MATMUL,
    )


def advance(*operands):
    return call(
        advance_kernel,
        (near(*TOKEN), vmem(*TOKEN, dtype=F32), vmem(TOKENS, 1, dtype=F32)),
        [vmem(*UNITS), vmem(HIDDEN, FEATURES), VECTOR, vmem(*TOKEN), vmem(*TOKEN), vmem(*TOKEN, dtype=F32)]
        + [sems(3), sems(CHUNKS), sems(CHUNKS)],
        operands,
        "fffff",
        MATMUL,
    )


def finish(*operands):
    return call(
        finish_kernel,
        pltpu.HBM(TOKEN, BF16),
        [BLOCKS, vmem(*TOKEN), sems(BATCHES)],
        operands,
        "nhhhh",
    )


def shards(
    state, spec_weight1, spec_bias1, spec_weight2, spec_bias2, norm1_gain, norm1_bias, norm2_gain, norm2_bias,
    fc1_weight, fc1_bias, fc2_weight, fc2_bias, cotangent,
):
    tokens = state.reshape(TOKEN)
    cot = cotangent.reshape(TOKEN)
    tables = map(jnp.asarray, (*width_tables(), *height_tables()))
    weight1, weight2 = spec_weight1.reshape(2, BLOCK, BLOCK), spec_weight2.reshape(2, BLOCK, BLOCK)
    bias1, bias2 = spec_bias1.reshape(2, BLOCK), spec_bias2.reshape(2, BLOCK)

    wire = begin(tokens, norm1_gain, norm1_bias)
    grad_hidden, base, cot, gain1, *held = gradient(
        cot, tokens, norm1_bias, fc2_weight, norm1_gain,
        *tables, weight1, weight2, bias1, bias2, norm2_gain, norm2_bias, fc1_bias.reshape(1, -1),
    )
    width_forward, width_inverse, height_forward, height_inverse, weight1, weight2, bias1, bias2 = held[:8]
    gain2, shift2, fc1_bias = held[8:]
    wire = to_lat(wire, width_forward)
    wire, slopes, squares = filtered(wire, height_forward, height_inverse, weight1, bias1, weight2, bias2)
    wire = to_lon(wire, width_inverse)
    hidden, mixed, grad_mixed, wire = token(wire, base, cot, gain2, shift2, fc1_bias, fc1_weight, grad_hidden)
    wire = to_lat(wire, width_forward)
    wire = adjoint(wire, height_forward, height_inverse, weight1, weight2, slopes, squares)
    advanced, normed, scale = advance(hidden, fc2_weight, fc2_bias, mixed, tokens)
    wire = to_lon(wire, width_inverse)
    sensitivity = finish(wire, normed, scale, grad_mixed, gain1)
    return advanced.reshape(state.shape), sensitivity.reshape(state.shape)


def solution(mesh):
    field = P("ens", "lat", "lon", None)
    block, bias = P(None, "lon", None, None), P(None, "lon", None)
    return jax.shard_map(
        shards,
        mesh=mesh,
        in_specs=(field, block, bias, block, bias, *[P()] * 8, field),
        out_specs=(field, field),
        check_vma=False,
    )
```

```python
import math

import jax
import jax.numpy as jnp
import numpy as np
from jax import lax
from jax.experimental import pallas as pl
from jax.experimental.pallas import tpu as pltpu
from jax.sharding import PartitionSpec as P

EPSILON = 1e-06
THRESHOLD = 0.01
LATS, LONS = 16, 8
HEIGHT, WIDTH, FEATURES, HIDDEN = 96, 192, 768, 3072
ROWS, COLS = HEIGHT // LATS, WIDTH // LONS
BLOCK = FEATURES // LONS
STATES = 2
GROUPS = STATES * ROWS
TOKENS = GROUPS * COLS
LANES = GROUPS * BLOCK
TILES = LANES // 128
WIRE = TILES * GROUPS
STRIDE = 109
CHUNK = 1024
STEP = 256
BATCH = 6
BATCHES = GROUPS // BATCH
CHUNKS = HIDDEN // CHUNK
F32, BF16 = jnp.float32, jnp.bfloat16


def split_table(table):
    high = table.astype(BF16)
    return np.stack([high, (table - high.astype(np.float64)).astype(BF16)])


def width_tables():
    part, q, d = np.meshgrid(np.arange(2), np.arange(ROWS), np.arange(LATS), indexing="ij")
    part, freq = part.reshape(-1, 1), (q + ROWS * d).reshape(-1, 1)
    w = np.arange(WIDTH).reshape(1, -1)
    angle = 2.0 * math.pi * (freq * w % WIDTH) / WIDTH
    parity = np.where(w % 2 == 0, 1.0, -1.0)
    scale = 1.0 / math.sqrt(WIDTH)
    forward = np.where(part == 0, np.cos(angle), np.where(freq == 0, parity, -np.sin(angle)))
    twice = np.where(freq == 0, 1.0, 2.0)
    return split_table(forward * scale), split_table((forward * twice * scale).T)


def height_tables():
    p = np.arange(HEIGHT).reshape(-1, 1, 1)
    r = np.arange(ROWS).reshape(1, -1, 1)
    s = np.arange(LATS).reshape(1, 1, -1)
    angle = 2.0 * math.pi * (p * (ROWS * s + r) % HEIGHT) / HEIGHT
    c, n = np.cos(angle) / math.sqrt(HEIGHT), np.sin(angle) / math.sqrt(HEIGHT)
    zero = np.zeros_like(c)

    def join(rows):
        return np.concatenate([np.stack(row, axis=2).reshape(HEIGHT, -1) for row in rows], axis=0)

    plain = join([[c, n], [c, n], [-n, c], [n, -c]])
    packed = join([[c, zero], [zero, c], [-n, zero], [zero, -n]])

    def join_back(rows):
        return np.concatenate(
            [np.concatenate([v.reshape(HEIGHT, -1).T for v in row], axis=1) for row in rows], axis=0
        )

    h = 0.5
    plain_back = join_back([[h * c, h * c, -h * n, h * n], [h * n, h * n, h * c, -h * c]])
    packed_back = join_back([[c, zero, -n, zero], [zero, c, zero, -n]])
    return np.stack([plain, packed]).astype(BF16), np.stack([plain_back, packed_back]).astype(BF16)


def dot(a, b):
    return lax.dot_general(a, b, (((1,), (0,)), ((), ())), preferred_element_type=F32)


def dot_t(a, b):
    return lax.dot_general(a, b, (((1,), (1,)), ((), ())), preferred_element_type=F32)


def lane_index(rows):
    return lax.broadcasted_iota(jnp.int32, (rows, 128), 1)


def unpack4(t0, t1, t2):
    lane = lane_index(t0.shape[0])
    b1 = jnp.where(lane < 32, pltpu.roll(t0, 32, 1), pltpu.roll(t1, 32, 1))
    b2 = jnp.where(lane < 64, pltpu.roll(t1, 64, 1), pltpu.roll(t2, 64, 1))
    return t0, b1, b2, pltpu.roll(t2, 96, 1)


def pack4(b0, b1, b2, b3):
    lane = lane_index(b0.shape[0])
    r1, r2, r3 = pltpu.roll(b1, 96, 1), pltpu.roll(b2, 64, 1), pltpu.roll(b3, 32, 1)
    return (
        jnp.where(lane < 96, b0, r1),
        jnp.where(lane < 64, r1, r2),
        jnp.where(lane < 32, r2, r3),
    )


def row(vector):
    return vector[...].reshape(1, -1)


def norm(values):
    average = jnp.mean(values, axis=-1, keepdims=True)
    centred = values - average
    inverse = lax.rsqrt(jnp.mean(centred * centred, axis=-1, keepdims=True) + EPSILON)
    return centred * inverse, inverse


def norm_backward(gradient, gain, normed, inverse):
    scaled = gradient * gain
    return inverse * (
        scaled
        - jnp.mean(scaled, axis=-1, keepdims=True)
        - normed * jnp.mean(scaled * normed, axis=-1, keepdims=True)
    )


def gelu_pair(values):
    cumulative = 0.5 * (1.0 + lax.erf(values * 0.7071067811865476))
    density = jnp.exp(-0.5 * values * values) * 0.3989422804014327
    return values * cumulative, cumulative + values * density


def scatter_blocks(blocks, batch, values):
    tiles = [values[:, 128 * i : 128 * i + 128] for i in range(6)]
    for j, b in enumerate((*unpack4(*tiles[:3]), *unpack4(*tiles[3:]))):
        for n in range(BATCH):
            blocks[j, BATCH * batch + n] = b[COLS * n : COLS * n + COLS]


def send_blocks(blocks, wire):
    for j in range(LONS):
        for g in range(GROUPS // 4):
            tiles = pack4(*(blocks[j, 4 * g + n] for n in range(4)))
            for i, t in enumerate(tiles):
                at = 384 * g + 128 * i
                wire[j, :, at : at + 128] = t.astype(BF16)


def receive_blocks(wire, blocks):
    for j in range(LONS):
        for g in range(GROUPS // 4):
            at = 384 * g
            tiles = [wire[j, :, at + 128 * i : at + 128 * i + 128].astype(F32) for i in range(3)]
            for n, b in enumerate(unpack4(*tiles)):
                blocks[j, 4 * g + n] = b


def gather_blocks(blocks, batch):
    groups = range(BATCH * batch, BATCH * batch + BATCH)
    parts = [jnp.concatenate([blocks[j, k] for k in groups], axis=0) for j in range(LONS)]
    return jnp.concatenate([*pack4(*parts[:4]), *pack4(*parts[4:])], axis=1)


def fetch(sem, *pairs):
    copies = [pltpu.make_async_copy(source, target, sem.at[n]) for n, (source, target) in enumerate(pairs)]
    for c in copies:
        c.start()

    def wait(*numbers):
        for n in numbers:
            copies[n].wait()

    return wait


def batch_rows(batch):
    size = BATCH * COLS
    return slice(size * batch, size * batch + size)


def begin_kernel(states, gains, shifts, wire, state, gain, shift, blocks, sem):
    fetch(sem, (states, state), (gains, gain), (shifts, shift))(0, 1, 2)
    for batch in range(BATCHES):
        normed, _ = norm(state[batch_rows(batch), :].astype(F32))
        value = (normed * row(gain) + row(shift)).astype(BF16)
        scatter_blocks(blocks, batch, value.astype(F32))
    send_blocks(blocks, wire)


def wire_out(scratch, wire):
    for d in range(LATS):
        wire[d] = scratch[STRIDE * d : STRIDE * d + WIRE, :].astype(BF16)


def wire_in(wire, scratch):
    for d in range(LATS):
        scratch[STRIDE * d : STRIDE * d + WIRE, :] = wire[d].astype(F32)


def peers(row):
    return pl.ds(row, LATS, stride=STRIDE)


def width_kernel(field, table, wire, scratch):
    product = dot(table[0], field[...]) + dot(table[1], field[...])
    for e in range(GROUPS):
        for i in range(TILES):
            scratch[peers(GROUPS * i + e), :] = product[16 * e : 16 * e + 16, 128 * i : 128 * i + 128]
    wire_out(scratch, wire)


def width_back_kernel(wire, table, field, scratch, gathered):
    wire_in(wire, scratch)
    for e in range(GROUPS):
        for i in range(TILES):
            piece = scratch[peers(GROUPS * i + e), :]
            gathered[16 * e : 16 * e + 16, 128 * i : 128 * i + 128] = piece.astype(BF16)
    field[...] = (dot(table[0], gathered[...]) + dot(table[1], gathered[...])).astype(BF16)


def spectrum_in(wire, scratch, columns):
    wire_in(wire, scratch)
    for part in range(2):
        for q in range(ROWS):
            e = ROWS * part + q
            for g in range(GROUPS // 4):
                tiles = [scratch[peers(GROUPS * (3 * g + i) + e), :] for i in range(3)]
                for n, b in enumerate(unpack4(*tiles)):
                    state, r = divmod(4 * g + n, ROWS)
                    at = 16 * (2 * r + part)
                    columns[q, at : at + 16, 128 * state : 128 * state + 128] = b.astype(BF16)


def spectrum_out(backs, scratch, wire):
    for part in range(2):
        for q in range(ROWS):
            e = ROWS * part + q
            for g in range(GROUPS // 4):
                blocks = []
                for n in range(4):
                    state, r = divmod(4 * g + n, ROWS)
                    at = 16 * (ROWS * part + r)
                    blocks.append(backs[q, at : at + 16, 128 * state : 128 * state + 128])
                for i, t in enumerate(pack4(*blocks)):
                    scratch[peers(GROUPS * (3 * g + i) + e), :] = t
    wire_out(scratch, wire)


def build_weight(weight, square, out):
    square[...] = jnp.zeros_like(square)
    square[0:BLOCK, 0:BLOCK] = weight[0]
    square[0:BLOCK, 128 : 128 + BLOCK] = weight[1]
    square[128 : 128 + BLOCK, 0:BLOCK] = -weight[1]
    square[128 : 128 + BLOCK, 128 : 128 + BLOCK] = weight[0]
    out[...] = square[...].astype(BF16)


def build_bias(bias, out):
    out[...] = jnp.zeros_like(out)
    out[0:1, 0:BLOCK] = bias[0:1, :]
    out[0:1, 128 : 128 + BLOCK] = bias[1:2, :]


def to_points(spectrum):
    half = 2 * HEIGHT
    return jnp.concatenate(
        [
            jnp.concatenate([spectrum[:half, at : at + 128], spectrum[half:, at : at + 128]], axis=1)
            for at in (0, 128)
        ],
        axis=0,
    )


def from_points(points):
    half = 2 * HEIGHT
    return jnp.concatenate(
        [
            jnp.concatenate([points[at : at + half, :128], points[at : at + half, 128:]], axis=0)
            for at in (0, half)
        ],
        axis=1,
    )


def is_packed(q):
    return jnp.where(lax.axis_index("lat") == 0, 1, 0) if q == 0 else 0


def filter_kernel(
    wire, forward, inverse, weight1, bias1, weight2, bias2, fc1s,
    wire_back, slopes_out, squares_out, fc1,
    slopes, squares, scratch, columns, backs, square, w1, w2, c1, c2, sem, sem_token,
):
    wait_token = fetch(sem_token, (fc1s, fc1))
    build_weight(weight1, square, w1)
    build_weight(weight2, square, w2)
    build_bias(bias1, c1)
    build_bias(bias2, c2)
    spectrum_in(wire, scratch, columns)

    for q in range(ROWS):
        which = is_packed(q)
        points = to_points(dot(forward[which], columns[q]).astype(BF16))
        active, slope = gelu_pair(dot(points, w1[...]) + c1[...])
        slopes[q] = slope.astype(BF16)
        post = dot(active.astype(BF16), w2[...]) + c2[...]
        bend = jnp.tanh(post * (1.0 / THRESHOLD))
        squares[q] = (bend * bend).astype(BF16)
        shrunk = from_points((post - THRESHOLD * bend).astype(BF16))
        backs[q] = dot(inverse[which], shrunk)

    keep = fetch(sem, (slopes, slopes_out), (squares, squares_out))
    spectrum_out(backs, scratch, wire_back)
    keep(0, 1)
    wait_token(0)


def adjoint_kernel(
    wire, forward, inverse, weight1, weight2, slopes, squares,
    wire_back,
    scratch, columns, backs, square, w1, w2,
):
    build_weight(weight1, square, w1)
    build_weight(weight2, square, w2)
    spectrum_in(wire, scratch, columns)

    for q in range(ROWS):
        which = is_packed(q)
        spectrum = dot(forward[which], columns[q])
        points = (to_points(spectrum) * squares[q].astype(F32)).astype(BF16)
        pre = (dot_t(points, w2[...]) * slopes[q].astype(F32)).astype(BF16)
        shrunk = from_points(dot_t(pre, w1[...]).astype(BF16))
        backs[q] = dot(inverse[which], shrunk)

    spectrum_out(backs, scratch, wire_back)


def pieces(n):
    return pl.ds(CHUNK * n if isinstance(n, int) else pl.multiple_of(CHUNK * n, CHUNK), CHUNK)


def chunk_copies(sem, copy):
    one = lambda n: pltpu.make_async_copy(*copy(pieces(n)), sem.at[n])
    return lambda n: one(n).start(), lambda n: one(n).wait()


def gradient_kernel(cotangents, states, shift1s, fc2s, gain1s, *refs):
    more, (grad_hiddens, base, cotangent), rest = refs[:HELD], refs[HELD : HELD + 3], refs[HELD + 3 :]
    gain1, held, (state, shift1, fc2, grad_hidden, sem, sem_in, sem_out) = rest[0], rest[1 : HELD + 1], rest[HELD + 1 :]
    wait = fetch(
        sem, (cotangents, cotangent), (states, state), (gain1s, gain1), (shift1s, shift1),
        *zip(more, held, strict=True),
    )
    start_in, wait_in = chunk_copies(sem_in, lambda c: (fc2s.at[c, :], fc2.at[c, :]))
    start_out, wait_out = chunk_copies(sem_out, lambda c: (grad_hidden.at[:, c], grad_hiddens.at[:, c]))
    pl.loop(0, CHUNKS)(start_in)
    wait(*range(4 + HELD))
    for batch in range(BATCHES):
        rows = batch_rows(batch)
        value = state[rows, :].astype(F32)
        normed, _ = norm(value)
        base[rows, :] = (normed * row(gain1) + row(shift1)).astype(BF16).astype(F32) + value

    @pl.loop(0, CHUNKS)
    def _(n):
        wait_in(n)
        grad_hidden[:, pieces(n)] = dot_t(cotangent[...], fc2[pieces(n), :]).astype(BF16)
        start_out(n)

    pl.loop(0, CHUNKS)(wait_out)


def token_kernel(
    wire, base, cotangent, gain, shift, bias1, fc1, grad_hidden,
    hiddens, mixeds, grad_mixed, wire_next,
    hidden, mixed, blocks, rows_in, grad_pre, grad_total, sem, sem_hidden,
):
    start_hidden, wait_hidden = chunk_copies(sem_hidden, lambda c: (hidden.at[:, c], hiddens.at[:, c]))

    receive_blocks(wire, blocks)
    for batch in range(BATCHES):
        rows = batch_rows(batch)
        value = (gather_blocks(blocks, batch) + base[rows, :]).astype(BF16)
        mixed[rows, :] = value
        normed, _ = norm(value.astype(F32))
        rows_in[rows, :] = (normed * row(gain) + row(shift)).astype(BF16)
    keep = fetch(sem, (mixed, mixeds))

    def units(n):
        return slice(STEP * n, STEP * n + STEP)

    def before(n):
        return dot(rows_in[...], fc1[:, units(n)]) + bias1[:, units(n)]

    hidden_pre = before(0)
    for n in range(HIDDEN // STEP):
        following = before(n + 1) if n + 1 < HIDDEN // STEP else None
        value, slope = gelu_pair(hidden_pre)
        hidden[:, units(n)] = value.astype(BF16)
        grad_pre[:, units(n)] = (grad_hidden[:, units(n)].astype(F32) * slope).astype(BF16)
        if (STEP * n + STEP) % CHUNK == 0:
            start_hidden(STEP * n // CHUNK)
        hidden_pre = following
    grad_total[...] = dot_t(grad_pre[...], fc1[...])

    for batch in range(BATCHES):
        rows = batch_rows(batch)
        normed, scale = norm(mixed[rows, :].astype(F32))
        grad = cotangent[rows, :].astype(F32) + norm_backward(grad_total[rows, :], row(gain), normed, scale)
        grad = grad.astype(BF16)
        grad_mixed[rows, :] = grad
        scatter_blocks(blocks, batch, grad.astype(F32))
    send_blocks(blocks, wire_next)
    keep(0)
    pl.loop(0, CHUNKS)(wait_hidden)


def advance_kernel(
    hiddens, fc2s, bias2s, mixeds, states,
    advanced, normed, scale,
    hidden, fc2, bias2, mixed, state, total, sem, sem_hidden, sem_fc2,
):
    wait = fetch(sem, (bias2s, bias2), (mixeds, mixed), (states, state))
    start_hidden, wait_hidden = chunk_copies(sem_hidden, lambda c: (hiddens.at[:, c], hidden.at[:, c]))
    start_fc2, wait_fc2 = chunk_copies(sem_fc2, lambda c: (fc2s.at[c, :], fc2.at[c, :]))

    @pl.loop(0, CHUNKS)
    def _(n):
        start_hidden(n)
        start_fc2(n)

    wait(0, 1, 2)
    for batch in range(BATCHES):
        rows = batch_rows(batch)
        normed[rows, :], scale[rows, :] = norm(state[rows, :].astype(F32))
    total[...] = mixed[...].astype(F32) + row(bias2)

    @pl.loop(0, CHUNKS)
    def _(n):
        wait_hidden(n)
        wait_fc2(n)
        total[...] += dot(hidden[:, pieces(n)], fc2[pieces(n), :])

    advanced[...] = total[...].astype(BF16)


def finish_kernel(wire, normed, scale, grad_mixed, gain, sensitivity, blocks, out, sem_out):
    receive_blocks(wire, blocks)
    copies = []
    for batch in range(BATCHES):
        rows = batch_rows(batch)
        grad = grad_mixed[rows, :].astype(F32)
        grad_lowered = gather_blocks(blocks, batch) + grad
        grad = grad + norm_backward(grad_lowered, row(gain), normed[rows, :], scale[rows, :])
        out[rows, :] = grad.astype(BF16)
        copies.append(pltpu.make_async_copy(out.at[rows, :], sensitivity.at[rows, :], sem_out.at[batch]))
        copies[-1].start()
    for c in copies:
        c.wait()


def near(*shape, dtype=BF16):
    return jax.ShapeDtypeStruct(shape, dtype)


def vmem(*shape, dtype=BF16):
    return pltpu.VMEM(shape, dtype)


def sems(n):
    return pltpu.SemaphoreType.DMA((n,))


LON_WIRE = near(LONS, COLS, LANES)
FIELD = near(WIDTH, LANES)
LAT_WIRE = near(LATS, WIRE, 128)
BLOCKS = vmem(LONS, GROUPS, COLS, 128, dtype=F32)
PEERS = vmem(LATS * STRIDE, 128, dtype=F32)
POINTS = (ROWS, 4 * HEIGHT, 256)
SPECTRAL = (
    PEERS,
    vmem(ROWS, 2 * HEIGHT, 256),
    vmem(ROWS, 2 * HEIGHT, 256, dtype=F32),
    vmem(256, 256, dtype=F32),
    vmem(256, 256),
    vmem(256, 256),
)
WIDE_BIAS = vmem(1, 256, dtype=F32)
TOKEN, UNITS = (TOKENS, FEATURES), (TOKENS, HIDDEN)
VECTOR = vmem(FEATURES, dtype=F32)
PARAMS = pltpu.CompilerParams(vmem_limit_bytes=40 * 1024 * 1024)
HELD = 11
MATMUL = 2 * TOKENS * FEATURES * HIDDEN


def place(space):
    return pl.BlockSpec() if space is None else pl.BlockSpec(memory_space=space)


def call(kernel, out_shape, scratch, operands, places, flops=0):
    single = not isinstance(out_shape, tuple)
    shapes = (out_shape,) if single else out_shape
    specs = tuple(place(None if isinstance(o, jax.ShapeDtypeStruct) else o.memory_space) for o in shapes)
    spaces = [{"f": pltpu.HBM, "h": pltpu.VMEM, "n": None}[p] for p in places]
    return pl.pallas_call(
        kernel,
        out_shape=out_shape,
        in_specs=[place(m) for m in spaces],
        out_specs=specs[0] if single else specs,
        scratch_shapes=scratch,
        name=kernel.__name__,
        compiler_params=PARAMS,
        cost_estimate=pl.CostEstimate(flops=flops, bytes_accessed=0, transcendentals=0),
    )(*(v if m is None else pltpu.with_memory_space_constraint(v, m) for v, m in zip(operands, spaces, strict=True)))


def exchange(value, axis):
    return lax.all_to_all(value, axis, split_axis=0, concat_axis=0, tiled=True)


def to_lat(wire, table):
    field = exchange(wire, "lon").reshape(WIDTH, LANES)
    return exchange(call(width_kernel, LAT_WIRE, [PEERS], [field, table], "nh"), "lat")


def to_lon(wire, table):
    scratch = [PEERS, vmem(WIDTH, LANES)]
    field = call(width_back_kernel, FIELD, scratch, [exchange(wire, "lat"), table], "nh")
    return exchange(field.reshape(LON_WIRE.shape), "lon")


def begin(*operands):
    return call(
        begin_kernel,
        LON_WIRE,
        [vmem(*TOKEN), VECTOR, VECTOR, BLOCKS, sems(3)],
        operands,
        "fff",
    )


def filtered(*operands):
    return call(
        filter_kernel,
        (LAT_WIRE, pltpu.HBM(POINTS, BF16), pltpu.HBM(POINTS, BF16), vmem(FEATURES, HIDDEN)),
        [vmem(*POINTS), vmem(*POINTS), *SPECTRAL, WIDE_BIAS, WIDE_BIAS, sems(2), sems(1)],
        operands,
        "nhhhhhhf",
    )


def adjoint(wire, *operands):
    return call(adjoint_kernel, LAT_WIRE, [*SPECTRAL], [wire, *operands], "nhhhhnn")


def gradient(cot, tokens, shift1, fc2, gain1, *arrays):
    return call(
        gradient_kernel,
        (pltpu.HBM(UNITS, BF16), vmem(*TOKEN, dtype=F32), vmem(*TOKEN))
        + tuple(vmem(*a.shape, dtype=a.dtype) for a in (gain1, *arrays)),
        [vmem(*TOKEN), VECTOR, vmem(HIDDEN, FEATURES), vmem(*UNITS), sems(4 + HELD), sems(CHUNKS), sems(CHUNKS)],
        [cot, tokens, shift1, fc2, gain1, *arrays],
        "fffff" + "f" * len(arrays),
        MATMUL,
    )


def token(*operands):
    return call(
        token_kernel,
        (pltpu.HBM(UNITS, BF16), pltpu.HBM(TOKEN, BF16), vmem(*TOKEN), LON_WIRE),
        [vmem(*UNITS), vmem(*TOKEN), BLOCKS, vmem(*TOKEN)]
        + [vmem(*UNITS), vmem(*TOKEN, dtype=F32), sems(1), sems(CHUNKS)],
        operands,
        "nhhhhhhh",
        2 * MATMUL,
    )


def advance(*operands):
    return call(
        advance_kernel,
        (near(*TOKEN), vmem(*TOKEN, dtype=F32), vmem(TOKENS, 1, dtype=F32)),
        [vmem(*UNITS), vmem(HIDDEN, FEATURES), VECTOR, vmem(*TOKEN), vmem(*TOKEN), vmem(*TOKEN, dtype=F32)]
        + [sems(3), sems(CHUNKS), sems(CHUNKS)],
        operands,
        "fffff",
        MATMUL,
    )


def finish(*operands):
    return call(
        finish_kernel,
        pltpu.HBM(TOKEN, BF16),
        [BLOCKS, vmem(*TOKEN), sems(BATCHES)],
        operands,
        "nhhhh",
    )


def shards(
    state, spec_weight1, spec_bias1, spec_weight2, spec_bias2, norm1_gain, norm1_bias, norm2_gain, norm2_bias,
    fc1_weight, fc1_bias, fc2_weight, fc2_bias, cotangent,
):
    tokens = state.reshape(TOKEN)
    cot = cotangent.reshape(TOKEN)
    tables = map(jnp.asarray, (*width_tables(), *height_tables()))
    weight1, weight2 = spec_weight1.reshape(2, BLOCK, BLOCK), spec_weight2.reshape(2, BLOCK, BLOCK)
    bias1, bias2 = spec_bias1.reshape(2, BLOCK), spec_bias2.reshape(2, BLOCK)

    wire = begin(tokens, norm1_gain, norm1_bias)
    grad_hidden, base, cot, gain1, *held = gradient(
        cot, tokens, norm1_bias, fc2_weight, norm1_gain,
        *tables, weight1, weight2, bias1, bias2, norm2_gain, norm2_bias, fc1_bias.reshape(1, -1),
    )
    width_forward, width_inverse, height_forward, height_inverse, weight1, weight2, bias1, bias2 = held[:8]
    gain2, shift2, fc1_bias = held[8:]
    wire = to_lat(wire, width_forward)
    wire, slopes, squares, fc1 = filtered(
        wire, height_forward, height_inverse, weight1, bias1, weight2, bias2, fc1_weight
    )
    wire = to_lon(wire, width_inverse)
    hidden, mixed, grad_mixed, wire = token(wire, base, cot, gain2, shift2, fc1_bias, fc1, grad_hidden)
    wire = to_lat(wire, width_forward)
    wire = adjoint(wire, height_forward, height_inverse, weight1, weight2, slopes, squares)
    advanced, normed, scale = advance(hidden, fc2_weight, fc2_bias, mixed, tokens)
    wire = to_lon(wire, width_inverse)
    sensitivity = finish(wire, normed, scale, grad_mixed, gain1)
    return advanced.reshape(state.shape), sensitivity.reshape(state.shape)


def solution(mesh):
    field = P("ens", "lat", "lon", None)
    block, bias = P(None, "lon", None, None), P(None, "lon", None)
    return jax.shard_map(
        shards,
        mesh=mesh,
        in_specs=(field, block, bias, block, bias, *[P()] * 8, field),
        out_specs=(field, field),
        check_vma=False,
    )
```

```python
import math

import jax
import jax.numpy as jnp
import numpy as np
from jax import lax
from jax.experimental import pallas as pl
from jax.experimental.pallas import tpu as pltpu
from jax.sharding import PartitionSpec as P

EPSILON = 1e-06
THRESHOLD = 0.01
LATS, LONS = 16, 8
HEIGHT, WIDTH, FEATURES, HIDDEN = 96, 192, 768, 3072
ROWS, COLS = HEIGHT // LATS, WIDTH // LONS
BLOCK = FEATURES // LONS
STATES = 2
GROUPS = STATES * ROWS
TOKENS = GROUPS * COLS
LANES = GROUPS * BLOCK
TILES = LANES // 128
WIRE = TILES * GROUPS
STRIDE = 109
CHUNK = 1024
STEP = 256
BATCH = 6
BATCHES = GROUPS // BATCH
CHUNKS = HIDDEN // CHUNK
F32, BF16 = jnp.float32, jnp.bfloat16


def split_table(table):
    high = table.astype(BF16)
    return np.stack([high, (table - high.astype(np.float64)).astype(BF16)])


def width_tables():
    part, q, d = np.meshgrid(np.arange(2), np.arange(ROWS), np.arange(LATS), indexing="ij")
    part, freq = part.reshape(-1, 1), (q + ROWS * d).reshape(-1, 1)
    w = np.arange(WIDTH).reshape(1, -1)
    angle = 2.0 * math.pi * (freq * w % WIDTH) / WIDTH
    parity = np.where(w % 2 == 0, 1.0, -1.0)
    scale = 1.0 / math.sqrt(WIDTH)
    forward = np.where(part == 0, np.cos(angle), np.where(freq == 0, parity, -np.sin(angle)))
    twice = np.where(freq == 0, 1.0, 2.0)
    return split_table(forward * scale), split_table((forward * twice * scale).T)


def height_tables():
    p = np.arange(HEIGHT).reshape(-1, 1, 1)
    r = np.arange(ROWS).reshape(1, -1, 1)
    s = np.arange(LATS).reshape(1, 1, -1)
    angle = 2.0 * math.pi * (p * (ROWS * s + r) % HEIGHT) / HEIGHT
    c, n = np.cos(angle) / math.sqrt(HEIGHT), np.sin(angle) / math.sqrt(HEIGHT)
    zero = np.zeros_like(c)

    def join(rows):
        return np.concatenate([np.stack(row, axis=2).reshape(HEIGHT, -1) for row in rows], axis=0)

    plain = join([[c, n], [c, n], [-n, c], [n, -c]])
    packed = join([[c, zero], [zero, c], [-n, zero], [zero, -n]])

    def join_back(rows):
        return np.concatenate(
            [np.concatenate([v.reshape(HEIGHT, -1).T for v in row], axis=1) for row in rows], axis=0
        )

    h = 0.5
    plain_back = join_back([[h * c, h * c, -h * n, h * n], [h * n, h * n, h * c, -h * c]])
    packed_back = join_back([[c, zero, -n, zero], [zero, c, zero, -n]])
    return np.stack([plain, packed]).astype(BF16), np.stack([plain_back, packed_back]).astype(BF16)


def dot(a, b):
    return lax.dot_general(a, b, (((1,), (0,)), ((), ())), preferred_element_type=F32)


def dot_t(a, b):
    return lax.dot_general(a, b, (((1,), (1,)), ((), ())), preferred_element_type=F32)


def lane_index(rows):
    return lax.broadcasted_iota(jnp.int32, (rows, 128), 1)


def unpack4(t0, t1, t2):
    lane = lane_index(t0.shape[0])
    b1 = jnp.where(lane < 32, pltpu.roll(t0, 32, 1), pltpu.roll(t1, 32, 1))
    b2 = jnp.where(lane < 64, pltpu.roll(t1, 64, 1), pltpu.roll(t2, 64, 1))
    return t0, b1, b2, pltpu.roll(t2, 96, 1)


def pack4(b0, b1, b2, b3):
    lane = lane_index(b0.shape[0])
    r1, r2, r3 = pltpu.roll(b1, 96, 1), pltpu.roll(b2, 64, 1), pltpu.roll(b3, 32, 1)
    return (
        jnp.where(lane < 96, b0, r1),
        jnp.where(lane < 64, r1, r2),
        jnp.where(lane < 32, r2, r3),
    )


def row(vector):
    return vector[...].reshape(1, -1)


def norm(values):
    average = jnp.mean(values, axis=-1, keepdims=True)
    centred = values - average
    inverse = lax.rsqrt(jnp.mean(centred * centred, axis=-1, keepdims=True) + EPSILON)
    return centred * inverse, inverse


def norm_backward(gradient, gain, normed, inverse):
    scaled = gradient * gain
    return inverse * (
        scaled
        - jnp.mean(scaled, axis=-1, keepdims=True)
        - normed * jnp.mean(scaled * normed, axis=-1, keepdims=True)
    )


def gelu_pair(values):
    cumulative = 0.5 * (1.0 + lax.erf(values * 0.7071067811865476))
    density = jnp.exp(-0.5 * values * values) * 0.3989422804014327
    return values * cumulative, cumulative + values * density


def scatter_blocks(blocks, batch, values):
    tiles = [values[:, 128 * i : 128 * i + 128] for i in range(6)]
    for j, b in enumerate((*unpack4(*tiles[:3]), *unpack4(*tiles[3:]))):
        for n in range(BATCH):
            blocks[j, BATCH * batch + n] = b[COLS * n : COLS * n + COLS]


def send_blocks(blocks, wire):
    for j in range(LONS):
        for g in range(GROUPS // 4):
            tiles = pack4(*(blocks[j, 4 * g + n] for n in range(4)))
            for i, t in enumerate(tiles):
                at = 384 * g + 128 * i
                wire[j, :, at : at + 128] = t.astype(BF16)


def receive_blocks(wire, blocks):
    for j in range(LONS):
        for g in range(GROUPS // 4):
            at = 384 * g
            tiles = [wire[j, :, at + 128 * i : at + 128 * i + 128].astype(F32) for i in range(3)]
            for n, b in enumerate(unpack4(*tiles)):
                blocks[j, 4 * g + n] = b


def gather_blocks(blocks, batch):
    groups = range(BATCH * batch, BATCH * batch + BATCH)
    parts = [jnp.concatenate([blocks[j, k] for k in groups], axis=0) for j in range(LONS)]
    return jnp.concatenate([*pack4(*parts[:4]), *pack4(*parts[4:])], axis=1)


def fetch(sem, *pairs):
    copies = [pltpu.make_async_copy(source, target, sem.at[n]) for n, (source, target) in enumerate(pairs)]
    for c in copies:
        c.start()

    def wait(*numbers):
        for n in numbers:
            copies[n].wait()

    return wait


def batch_rows(batch):
    size = BATCH * COLS
    return slice(size * batch, size * batch + size)


def begin_kernel(states, gains, shifts, wire, state, gain, shift, blocks, sem):
    fetch(sem, (states, state), (gains, gain), (shifts, shift))(0, 1, 2)
    for batch in range(BATCHES):
        normed, _ = norm(state[batch_rows(batch), :].astype(F32))
        value = (normed * row(gain) + row(shift)).astype(BF16)
        scatter_blocks(blocks, batch, value.astype(F32))
    send_blocks(blocks, wire)


def wire_out(scratch, wire):
    for d in range(LATS):
        wire[d] = scratch[STRIDE * d : STRIDE * d + WIRE, :].astype(BF16)


def wire_in(wire, scratch):
    for d in range(LATS):
        scratch[STRIDE * d : STRIDE * d + WIRE, :] = wire[d].astype(F32)


def peers(row):
    return pl.ds(row, LATS, stride=STRIDE)


def width_kernel(field, table, wire, scratch):
    product = dot(table[0], field[...]) + dot(table[1], field[...])
    for e in range(GROUPS):
        for i in range(TILES):
            scratch[peers(GROUPS * i + e), :] = product[16 * e : 16 * e + 16, 128 * i : 128 * i + 128]
    wire_out(scratch, wire)


def width_back_kernel(wire, table, field, scratch, gathered):
    wire_in(wire, scratch)
    for e in range(GROUPS):
        for i in range(TILES):
            piece = scratch[peers(GROUPS * i + e), :]
            gathered[16 * e : 16 * e + 16, 128 * i : 128 * i + 128] = piece.astype(BF16)
    field[...] = (dot(table[0], gathered[...]) + dot(table[1], gathered[...])).astype(BF16)


def spectrum_in(wire, scratch, columns):
    wire_in(wire, scratch)
    for part in range(2):
        for q in range(ROWS):
            e = ROWS * part + q
            for g in range(GROUPS // 4):
                tiles = [scratch[peers(GROUPS * (3 * g + i) + e), :] for i in range(3)]
                for n, b in enumerate(unpack4(*tiles)):
                    state, r = divmod(4 * g + n, ROWS)
                    at = 16 * (2 * r + part)
                    columns[q, at : at + 16, 128 * state : 128 * state + 128] = b.astype(BF16)


def spectrum_out(backs, scratch, wire):
    for part in range(2):
        for q in range(ROWS):
            e = ROWS * part + q
            for g in range(GROUPS // 4):
                blocks = []
                for n in range(4):
                    state, r = divmod(4 * g + n, ROWS)
                    at = 16 * (ROWS * part + r)
                    blocks.append(backs[q, at : at + 16, 128 * state : 128 * state + 128])
                for i, t in enumerate(pack4(*blocks)):
                    scratch[peers(GROUPS * (3 * g + i) + e), :] = t
    wire_out(scratch, wire)


def build_weight(weight, square, out):
    square[...] = jnp.zeros_like(square)
    square[0:BLOCK, 0:BLOCK] = weight[0]
    square[0:BLOCK, 128 : 128 + BLOCK] = weight[1]
    square[128 : 128 + BLOCK, 0:BLOCK] = -weight[1]
    square[128 : 128 + BLOCK, 128 : 128 + BLOCK] = weight[0]
    out[...] = square[...].astype(BF16)


def build_bias(bias, out):
    out[...] = jnp.zeros_like(out)
    out[0:1, 0:BLOCK] = bias[0:1, :]
    out[0:1, 128 : 128 + BLOCK] = bias[1:2, :]


def to_points(spectrum):
    half = 2 * HEIGHT
    return jnp.concatenate(
        [
            jnp.concatenate([spectrum[:half, at : at + 128], spectrum[half:, at : at + 128]], axis=1)
            for at in (0, 128)
        ],
        axis=0,
    )


def from_points(points):
    half = 2 * HEIGHT
    return jnp.concatenate(
        [
            jnp.concatenate([points[at : at + half, :128], points[at : at + half, 128:]], axis=0)
            for at in (0, half)
        ],
        axis=1,
    )


def is_packed(q):
    return jnp.where(lax.axis_index("lat") == 0, 1, 0) if q == 0 else 0


def filter_kernel(
    wire, forward, inverse, weight1, bias1, weight2, bias2, fc1s,
    wire_back, slopes_out, squares_out, fc1,
    slopes, squares, scratch, columns, backs, square, w1, w2, c1, c2, sem, sem_token,
):
    wait_token = fetch(sem_token, (fc1s, fc1))
    build_weight(weight1, square, w1)
    build_weight(weight2, square, w2)
    build_bias(bias1, c1)
    build_bias(bias2, c2)
    spectrum_in(wire, scratch, columns)

    for q in range(ROWS):
        which = is_packed(q)
        points = to_points(dot(forward[which], columns[q]).astype(BF16))
        active, slope = gelu_pair(dot(points, w1[...]) + c1[...])
        slopes[q] = slope.astype(BF16)
        post = dot(active.astype(BF16), w2[...]) + c2[...]
        bend = jnp.tanh(post * (1.0 / THRESHOLD))
        squares[q] = (bend * bend).astype(BF16)
        shrunk = from_points((post - THRESHOLD * bend).astype(BF16))
        backs[q] = dot(inverse[which], shrunk)

    keep = fetch(sem, (slopes, slopes_out), (squares, squares_out))
    spectrum_out(backs, scratch, wire_back)
    keep(0, 1)
    wait_token(0)


def adjoint_kernel(
    wire, forward, inverse, weight1, weight2, slopes, squares,
    wire_back,
    scratch, columns, backs, square, w1, w2,
):
    build_weight(weight1, square, w1)
    build_weight(weight2, square, w2)
    spectrum_in(wire, scratch, columns)

    for q in range(ROWS):
        which = is_packed(q)
        spectrum = dot(forward[which], columns[q])
        points = (to_points(spectrum) * squares[q].astype(F32)).astype(BF16)
        pre = (dot_t(points, w2[...]) * slopes[q].astype(F32)).astype(BF16)
        shrunk = from_points(dot_t(pre, w1[...]).astype(BF16))
        backs[q] = dot(inverse[which], shrunk)

    spectrum_out(backs, scratch, wire_back)


def pieces(n):
    return pl.ds(CHUNK * n if isinstance(n, int) else pl.multiple_of(CHUNK * n, CHUNK), CHUNK)


def chunk_copies(sem, copy):
    one = lambda n: pltpu.make_async_copy(*copy(pieces(n)), sem.at[n])
    return lambda n: one(n).start(), lambda n: one(n).wait()


def gradient_kernel(cotangents, states, shift1s, fc2s, gain1s, *refs):
    more, (grad_hiddens, base, cotangent), rest = refs[:HELD], refs[HELD : HELD + 3], refs[HELD + 3 :]
    gain1, held, (state, shift1, fc2, grad_hidden, sem, sem_in, sem_out) = rest[0], rest[1 : HELD + 1], rest[HELD + 1 :]
    wait = fetch(
        sem, (cotangents, cotangent), (states, state), (gain1s, gain1), (shift1s, shift1),
        *zip(more, held, strict=True),
    )
    start_in, wait_in = chunk_copies(sem_in, lambda c: (fc2s.at[c, :], fc2.at[c, :]))
    start_out, wait_out = chunk_copies(sem_out, lambda c: (grad_hidden.at[:, c], grad_hiddens.at[:, c]))
    pl.loop(0, CHUNKS)(start_in)
    wait(*range(4 + HELD))
    for batch in range(BATCHES):
        rows = batch_rows(batch)
        value = state[rows, :].astype(F32)
        normed, _ = norm(value)
        base[rows, :] = (normed * row(gain1) + row(shift1)).astype(BF16).astype(F32) + value

    @pl.loop(0, CHUNKS)
    def _(n):
        wait_in(n)
        grad_hidden[:, pieces(n)] = dot_t(cotangent[...], fc2[pieces(n), :]).astype(BF16)
        start_out(n)

    pl.loop(0, CHUNKS)(wait_out)


def token_kernel(
    wire, base, cotangent, gain, shift, bias1, fc1, grad_hidden,
    hiddens, mixeds, grad_mixed, wire_next,
    hidden, mixed, blocks, rows_in, grad_pre, grad_total, sem, sem_hidden,
):
    start_hidden, wait_hidden = chunk_copies(sem_hidden, lambda c: (hidden.at[:, c], hiddens.at[:, c]))

    receive_blocks(wire, blocks)
    for batch in range(BATCHES):
        rows = batch_rows(batch)
        value = (gather_blocks(blocks, batch) + base[rows, :]).astype(BF16)
        mixed[rows, :] = value
        normed, _ = norm(value.astype(F32))
        rows_in[rows, :] = (normed * row(gain) + row(shift)).astype(BF16)
    keep = fetch(sem, (mixed, mixeds))

    def units(n):
        return slice(STEP * n, STEP * n + STEP)

    def before(n):
        return dot(rows_in[...], fc1[:, units(n)]) + bias1[:, units(n)]

    hidden_pre = before(0)
    for n in range(HIDDEN // STEP):
        following = before(n + 1) if n + 1 < HIDDEN // STEP else None
        value, slope = gelu_pair(hidden_pre)
        hidden[:, units(n)] = value.astype(BF16)
        grad_pre[:, units(n)] = (grad_hidden[:, units(n)].astype(F32) * slope).astype(BF16)
        if (STEP * n + STEP) % CHUNK == 0:
            start_hidden(STEP * n // CHUNK)
        hidden_pre = following
    grad_total[...] = dot_t(grad_pre[...], fc1[...])

    for batch in range(BATCHES):
        rows = batch_rows(batch)
        normed, scale = norm(mixed[rows, :].astype(F32))
        grad = cotangent[rows, :].astype(F32) + norm_backward(grad_total[rows, :], row(gain), normed, scale)
        grad = grad.astype(BF16)
        grad_mixed[rows, :] = grad
        scatter_blocks(blocks, batch, grad.astype(F32))
    send_blocks(blocks, wire_next)
    keep(0)
    pl.loop(0, CHUNKS)(wait_hidden)


def advance_kernel(
    hiddens, fc2s, bias2s, mixeds, states,
    advanced, normed, scale,
    hidden, fc2, bias2, mixed, state, total, sem, sem_hidden, sem_fc2,
):
    wait = fetch(sem, (bias2s, bias2), (mixeds, mixed), (states, state))
    start_hidden, wait_hidden = chunk_copies(sem_hidden, lambda c: (hiddens.at[:, c], hidden.at[:, c]))
    start_fc2, wait_fc2 = chunk_copies(sem_fc2, lambda c: (fc2s.at[c, :], fc2.at[c, :]))

    @pl.loop(0, CHUNKS)
    def _(n):
        start_hidden(n)
        start_fc2(n)

    wait(0, 1, 2)
    for batch in range(BATCHES):
        rows = batch_rows(batch)
        normed[rows, :], scale[rows, :] = norm(state[rows, :].astype(F32))
    total[...] = mixed[...].astype(F32) + row(bias2)

    @pl.loop(0, CHUNKS)
    def _(n):
        wait_hidden(n)
        wait_fc2(n)
        total[...] += dot(hidden[:, pieces(n)], fc2[pieces(n), :])

    advanced[...] = total[...].astype(BF16)


def finish_kernel(wire, normed, scale, grad_mixed, gain, sensitivity, blocks, out, sem_out):
    receive_blocks(wire, blocks)
    copies = []
    for batch in range(BATCHES):
        rows = batch_rows(batch)
        grad = grad_mixed[rows, :].astype(F32)
        grad_lowered = gather_blocks(blocks, batch) + grad
        grad = grad + norm_backward(grad_lowered, row(gain), normed[rows, :], scale[rows, :])
        out[rows, :] = grad.astype(BF16)
        copies.append(pltpu.make_async_copy(out.at[rows, :], sensitivity.at[rows, :], sem_out.at[batch]))
        copies[-1].start()
    for c in copies:
        c.wait()


def near(*shape, dtype=BF16):
    return jax.ShapeDtypeStruct(shape, dtype)


def vmem(*shape, dtype=BF16):
    return pltpu.VMEM(shape, dtype)


def sems(n):
    return pltpu.SemaphoreType.DMA((n,))


LON_WIRE = near(LONS, COLS, LANES)
FIELD = near(WIDTH, LANES)
LAT_WIRE = near(LATS, WIRE, 128)
BLOCKS = vmem(LONS, GROUPS, COLS, 128, dtype=F32)
PEERS = vmem(LATS * STRIDE + 15, 128, dtype=F32)
POINTS = (ROWS, 4 * HEIGHT, 256)
SPECTRAL = (
    PEERS,
    vmem(ROWS, 2 * HEIGHT, 256),
    vmem(ROWS, 2 * HEIGHT, 256, dtype=F32),
    vmem(256, 256, dtype=F32),
    vmem(256, 256),
    vmem(256, 256),
)
WIDE_BIAS = vmem(1, 256, dtype=F32)
TOKEN, UNITS = (TOKENS, FEATURES), (TOKENS, HIDDEN)
VECTOR = vmem(FEATURES, dtype=F32)
PARAMS = pltpu.CompilerParams(vmem_limit_bytes=40 * 1024 * 1024)
HELD = 11
MATMUL = 2 * TOKENS * FEATURES * HIDDEN


def place(space):
    return pl.BlockSpec() if space is None else pl.BlockSpec(memory_space=space)


def call(kernel, out_shape, scratch, operands, places, flops=0):
    single = not isinstance(out_shape, tuple)
    shapes = (out_shape,) if single else out_shape
    specs = tuple(place(None if isinstance(o, jax.ShapeDtypeStruct) else o.memory_space) for o in shapes)
    spaces = [{"f": pltpu.HBM, "h": pltpu.VMEM, "n": None}[p] for p in places]
    return pl.pallas_call(
        kernel,
        out_shape=out_shape,
        in_specs=[place(m) for m in spaces],
        out_specs=specs[0] if single else specs,
        scratch_shapes=scratch,
        name=kernel.__name__,
        compiler_params=PARAMS,
        cost_estimate=pl.CostEstimate(flops=flops, bytes_accessed=0, transcendentals=0),
    )(*(v if m is None else pltpu.with_memory_space_constraint(v, m) for v, m in zip(operands, spaces, strict=True)))


def exchange(value, axis):
    return lax.all_to_all(value, axis, split_axis=0, concat_axis=0, tiled=True)


def to_lat(wire, table):
    field = exchange(wire, "lon").reshape(WIDTH, LANES)
    return exchange(call(width_kernel, LAT_WIRE, [PEERS], [field, table], "nh"), "lat")


def to_lon(wire, table):
    scratch = [PEERS, vmem(WIDTH, LANES)]
    field = call(width_back_kernel, FIELD, scratch, [exchange(wire, "lat"), table], "nh")
    return exchange(field.reshape(LON_WIRE.shape), "lon")


def begin(*operands):
    return call(
        begin_kernel,
        LON_WIRE,
        [vmem(*TOKEN), VECTOR, VECTOR, BLOCKS, sems(3)],
        operands,
        "fff",
    )


def filtered(*operands):
    return call(
        filter_kernel,
        (LAT_WIRE, pltpu.HBM(POINTS, BF16), pltpu.HBM(POINTS, BF16), vmem(FEATURES, HIDDEN)),
        [vmem(*POINTS), vmem(*POINTS), *SPECTRAL, WIDE_BIAS, WIDE_BIAS, sems(2), sems(1)],
        operands,
        "nhhhhhhf",
    )


def adjoint(wire, *operands):
    return call(adjoint_kernel, LAT_WIRE, [*SPECTRAL], [wire, *operands], "nhhhhnn")


def gradient(cot, tokens, shift1, fc2, gain1, *arrays):
    return call(
        gradient_kernel,
        (pltpu.HBM(UNITS, BF16), vmem(*TOKEN, dtype=F32), vmem(*TOKEN))
        + tuple(vmem(*a.shape, dtype=a.dtype) for a in (gain1, *arrays)),
        [vmem(*TOKEN), VECTOR, vmem(HIDDEN, FEATURES), vmem(*UNITS), sems(4 + HELD), sems(CHUNKS), sems(CHUNKS)],
        [cot, tokens, shift1, fc2, gain1, *arrays],
        "fffff" + "f" * len(arrays),
        MATMUL,
    )


def token(*operands):
    return call(
        token_kernel,
        (pltpu.HBM(UNITS, BF16), pltpu.HBM(TOKEN, BF16), vmem(*TOKEN), LON_WIRE),
        [vmem(*UNITS), vmem(*TOKEN), BLOCKS, vmem(*TOKEN)]
        + [vmem(*UNITS), vmem(*TOKEN, dtype=F32), sems(1), sems(CHUNKS)],
        operands,
        "nhhhhhhh",
        2 * MATMUL,
    )


def advance(*operands):
    return call(
        advance_kernel,
        (near(*TOKEN), vmem(*TOKEN, dtype=F32), vmem(TOKENS, 1, dtype=F32)),
        [vmem(*UNITS), vmem(HIDDEN, FEATURES), VECTOR, vmem(*TOKEN), vmem(*TOKEN), vmem(*TOKEN, dtype=F32)]
        + [sems(3), sems(CHUNKS), sems(CHUNKS)],
        operands,
        "fffff",
        MATMUL,
    )


def finish(*operands):
    return call(
        finish_kernel,
        pltpu.HBM(TOKEN, BF16),
        [BLOCKS, vmem(*TOKEN), sems(BATCHES)],
        operands,
        "nhhhh",
    )


def shards(
    state, spec_weight1, spec_bias1, spec_weight2, spec_bias2, norm1_gain, norm1_bias, norm2_gain, norm2_bias,
    fc1_weight, fc1_bias, fc2_weight, fc2_bias, cotangent,
):
    tokens = state.reshape(TOKEN)
    cot = cotangent.reshape(TOKEN)
    tables = map(jnp.asarray, (*width_tables(), *height_tables()))
    weight1, weight2 = spec_weight1.reshape(2, BLOCK, BLOCK), spec_weight2.reshape(2, BLOCK, BLOCK)
    bias1, bias2 = spec_bias1.reshape(2, BLOCK), spec_bias2.reshape(2, BLOCK)

    wire = begin(tokens, norm1_gain, norm1_bias)
    grad_hidden, base, cot, gain1, *held = gradient(
        cot, tokens, norm1_bias, fc2_weight, norm1_gain,
        *tables, weight1, weight2, bias1, bias2, norm2_gain, norm2_bias, fc1_bias.reshape(1, -1),
    )
    width_forward, width_inverse, height_forward, height_inverse, weight1, weight2, bias1, bias2 = held[:8]
    gain2, shift2, fc1_bias = held[8:]
    wire = to_lat(wire, width_forward)
    wire, slopes, squares, fc1 = filtered(
        wire, height_forward, height_inverse, weight1, bias1, weight2, bias2, fc1_weight
    )
    wire = to_lon(wire, width_inverse)
    hidden, mixed, grad_mixed, wire = token(wire, base, cot, gain2, shift2, fc1_bias, fc1, grad_hidden)
    wire = to_lat(wire, width_forward)
    wire = adjoint(wire, height_forward, height_inverse, weight1, weight2, slopes, squares)
    advanced, normed, scale = advance(hidden, fc2_weight, fc2_bias, mixed, tokens)
    wire = to_lon(wire, width_inverse)
    sensitivity = finish(wire, normed, scale, grad_mixed, gain1)
    return advanced.reshape(state.shape), sensitivity.reshape(state.shape)


def solution(mesh):
    field = P("ens", "lat", "lon", None)
    block, bias = P(None, "lon", None, None), P(None, "lon", None)
    return jax.shard_map(
        shards,
        mesh=mesh,
        in_specs=(field, block, bias, block, bias, *[P()] * 8, field),
        out_specs=(field, field),
        check_vma=False,
    )
```
